32 devices in a mesh: gx: 4 (over z), gy: 8 (over y, x, core).
Axes of the slice: x: 2, y: 2, z: 4, core: 2. Of those that a mesh axis runs over, the one named last changes fastest.
Arguments:
- velocity: float32 [3, 32, 64, 1024], P(None, None, 'gx', 'gy'), may hold values from -6 to 6
- old_tendency: float32 [3, 32, 64, 1024], P(None, None, 'gx', 'gy'), may hold values from -6 to 6
- obstacle: int32 [32, 64, 1024], P(None, 'gx', 'gy'), may hold values 0 or 1
Outputs:
- corrected: float32 [3, 32, 64, 1024], P(None, None, 'gx', 'gy')
- pressure: float32 [32, 64, 1024], P(None, 'gx', 'gy')
The draws below stay inside these ranges and needn't reach their ends.
Inputs may be any that keep to these rules, and one draw needn't show every extreme that they name: `obstacle`: 1 marks a building cell, 0 a fluid cell.
All inputs are finite; a program needn't handle non-finite values. No bound on the sum of `obstacle` on one device may be relied on, other than what follows from the above.
Results may differ from the reference program's by a relative error of at most 0.00002.
Values sent between devices are 32-bit elements; how exact they have to be, the bound alone decides.
A program may use at most 128 MiB of HBM per device.

```python
import jax
import jax.numpy as jnp

NZ = 32
LEVELS = 3
SWEEPS = 2
COARSE_SWEEPS = 8
NX = 64
NY = 1024


def with_ends(entries, stream_key, least, largest):
    dims = entries.shape
    spot = [jax.random.randint(jax.random.fold_in(stream_key, axis), (), 0, dims[axis]) for axis in range(len(dims))]
    entries = entries.at[tuple(spot)].set(least)
    longest = dims.index(max(dims))
    spot[longest] = (spot[longest] + 1) % dims[longest]
    return entries.at[tuple(spot)].set(largest)


def level_of(own_key, shape, cuts, low, top_value):
    def one(dim, parts):
        heights = jax.random.uniform(jax.random.fold_in(jax.random.fold_in(own_key, 6), dim), (parts,), jnp.float32, low / len(cuts), top_value / len(cuts))
        return jnp.repeat(jnp.exp(heights), shape[dim] // parts).reshape((-1,) + (1,) * (len(shape) - dim - 1))

    gain = one(*cuts[0])
    for cut in cuts[1:]:
        gain = gain * one(*cut)
    return gain


def noise(rng, dims, spread, bound, cuts=(), held_as=jnp.bfloat16):
    values = jax.random.normal(rng, dims, jnp.float32) * spread
    if len(cuts) > 0:
        values = level_of(rng, dims, cuts, -0.22, 0.18) * values
    return jnp.clip(values, min=-bound, max=bound).astype(held_as)


def setup_inputs(seed: int = 0) -> dict:
    key_list = jax.random.split(jax.random.key(seed), 4)
    velocity = noise(key_list[0], (3, NZ, NX, NY), 1.0, 6.0, ((2, 4), (3, 8)), jnp.float32)
    old_tendency = noise(key_list[1], (3, NZ, NX, NY), 1.0, 6.0, ((2, 4), (3, 8)), jnp.float32)
    obstacle = with_ends((jax.random.randint(key_list[2], (NZ, NX, NY), 0, 6) < 1).astype(jnp.int32), jax.random.fold_in(key_list[2], 1), 0, 1)
    return {"velocity": velocity, "old_tendency": old_tendency, "obstacle": obstacle}


VISCOSITY = 0.1
TIME_STEP = 0.25
WEIGHT_NEW = 15.0 / 16.0
WEIGHT_OLD = -25.0 / 48.0
HELMHOLTZ = 1.0e-4


def vertical_pair(field):
    zeros_layer = jnp.zeros_like(field[..., :1, :, :])
    upper_cell = jnp.concatenate([field[..., 1:, :, :], zeros_layer], axis=-3)
    lower_cell = jnp.concatenate([zeros_layer, field[..., :-1, :, :]], axis=-3)
    return upper_cell, lower_cell


def vertical_count(size_z):
    layers = jnp.arange(size_z)
    above_ok = (layers < size_z - 1).astype(jnp.float32)
    below_ok = (layers > 0).astype(jnp.float32)
    return (above_ok + below_ok)[:, None, None]


def parity(size_z, size_x, size_y, start_x, start_y):
    layer_z = jnp.arange(size_z, dtype=jnp.int32)[:, None, None]
    row_x = (jnp.arange(size_x, dtype=jnp.int32) + start_x)[None, :, None]
    col_y = (jnp.arange(size_y, dtype=jnp.int32) + start_y)[None, None, :]
    return (layer_z + row_x + col_y) % 2


def gather_neighbours(extended):
    center = extended[:, 1:-1, 1:-1]
    upper_cell, lower_cell = vertical_pair(center)
    neighbours = extended[:, 2:, 1:-1] + extended[:, :-2, 1:-1] + extended[:, 1:-1, 2:] + extended[:, 1:-1, :-2] + upper_cell + lower_cell
    return center, neighbours


def relax_update(extended, source, spacing):
    center, neighbours = gather_neighbours(extended)
    diagonal = HELMHOLTZ + (4.0 + vertical_count(center.shape[0])) / spacing
    return (source + neighbours / spacing) / diagonal


def apply_operator(extended, spacing):
    center, neighbours = gather_neighbours(extended)
    diagonal = HELMHOLTZ + (4.0 + vertical_count(center.shape[0])) / spacing
    return diagonal * center - neighbours / spacing


def wrapped(field):
    return jnp.pad(field, ((0, 0), (1, 1), (1, 1)), mode="wrap")


def restrict(field):
    size_z, size_x, size_y = field.shape
    return field.reshape(size_z // 2, 2, size_x // 2, 2, size_y // 2, 2).mean(axis=(1, 3, 5))


def prolong(field):
    return jnp.repeat(jnp.repeat(jnp.repeat(field, 2, axis=0), 2, axis=1), 2, axis=2)


def global_sweep(field, source, spacing, colour):
    for shade in (0, 1):
        field = jnp.where(colour == shade, relax_update(wrapped(field), source, spacing), field)
    return field


def global_cycle(source, level):
    spacing = float(4 ** level)
    size_z, size_x, size_y = source.shape
    colour = parity(size_z, size_x, size_y, 0, 0)
    field = jnp.zeros_like(source)
    if level == LEVELS:
        for repeat_idx in range(COARSE_SWEEPS):
            field = global_sweep(field, source, spacing, colour)
        return field
    for repeat_idx in range(SWEEPS):
        field = global_sweep(field, source, spacing, colour)
    remain = source - apply_operator(wrapped(field), spacing)
    field = field + prolong(global_cycle(restrict(remain), level + 1))
    for repeat_idx in range(SWEEPS):
        field = global_sweep(field, source, spacing, colour)
    return field


def momentum(velocity, plus_x, minus_x, plus_y, minus_y, old_tendency, fluid):
    upper_cell, lower_cell = vertical_pair(velocity)
    advect = velocity[0] * (plus_x - minus_x) * 0.5 + velocity[1] * (plus_y - minus_y) * 0.5 + velocity[2] * (upper_cell - lower_cell) * 0.5
    diffuse = plus_x + minus_x + plus_y + minus_y + upper_cell + lower_cell - 6.0 * velocity
    tendency = VISCOSITY * diffuse - advect
    return fluid * (velocity + TIME_STEP * (WEIGHT_NEW * tendency + WEIGHT_OLD * old_tendency))


def divergence_of(east_u, west_u, north_v, south_v, predicted):
    upper_cell, lower_cell = vertical_pair(predicted[2])
    return 0.5 * ((east_u - west_u) + (north_v - south_v) + (upper_cell - lower_cell))


def correct(predicted, pressure_ext, pressure, fluid):
    upper_cell, lower_cell = vertical_pair(pressure)
    gradient = jnp.stack([
        0.5 * (pressure_ext[:, 2:, 1:-1] - pressure_ext[:, :-2, 1:-1]),
        0.5 * (pressure_ext[:, 1:-1, 2:] - pressure_ext[:, 1:-1, :-2]),
        0.5 * (upper_cell - lower_cell)])
    return fluid * (predicted - TIME_STEP * gradient)


def reference(velocity, old_tendency, obstacle):
    fluid = (1 - obstacle).astype(jnp.float32)
    predicted = momentum(velocity, jnp.roll(velocity, -1, axis=2), jnp.roll(velocity, 1, axis=2),
                         jnp.roll(velocity, -1, axis=3), jnp.roll(velocity, 1, axis=3), old_tendency, fluid)
    divergence = divergence_of(jnp.roll(predicted[0], -1, axis=1), jnp.roll(predicted[0], 1, axis=1),
                               jnp.roll(predicted[1], -1, axis=2), jnp.roll(predicted[1], 1, axis=2), predicted)
    source = -divergence / TIME_STEP
    pressure = global_cycle(source, 0)
    corrected = correct(predicted, wrapped(pressure), pressure, fluid)
    return corrected, pressure
```

```python
import functools

import jax
import jax.numpy as jnp
from jax import lax
from jax.experimental import pallas as pl
from jax.experimental.pallas import tpu as pltpu
from jax.sharding import PartitionSpec as P

LEVELS = 3
SWEEPS = 2
COARSE_SWEEPS = 8
VISCOSITY = 0.1
TIME_STEP = 0.25
WEIGHT_NEW = 15.0 / 16.0
WEIGHT_OLD = -25.0 / 48.0
HELMHOLTZ = 0.0001

LANES = 128
SUB = 8
HALO_X = 8
HALO_Y = 8
HALO_1 = 16
MESH = pl.DeviceIdType.MESH


def iota2(shape, dim):
    return lax.broadcasted_iota(jnp.int32, shape, dim)


def mm(a, b):
    return jnp.dot(a, b, precision=lax.Precision.HIGHEST, preferred_element_type=jnp.float32)


class Level:
    def __init__(self, level, nz):
        self.nz = nz
        self.scale = 1.0 / float(4**level)
        lane = iota2((SUB, LANES), 1)
        row = iota2((SUB, LANES), 0)
        self.lane = lane
        self.row = row
        z = lane % nz
        self.not_top = z < nz - 1
        self.not_bottom = z > 0
        parity = (z + lane // nz + row) % 2
        self.colour = [parity == 0, parity == 1]
        edge = (z == 0) | (z == nz - 1)
        diag_in = HELMHOLTZ + 6.0 * self.scale
        diag_edge = HELMHOLTZ + 5.0 * self.scale
        self.diag = jnp.where(edge, diag_edge, diag_in).astype(jnp.float32)
        self.inv = jnp.where(edge, 1.0 / diag_edge, 1.0 / diag_in).astype(jnp.float32)
        self.take = jnp.where(
            edge, self.scale / diag_edge, self.scale / diag_in
        ).astype(jnp.float32)

    def x_plus(self, tiles, t):
        n = len(tiles)
        both = tiles[t] if n == 1 else jnp.where(self.lane < self.nz, tiles[(t + 1) % n], tiles[t])
        return pltpu.roll(both, LANES - self.nz, 1)

    def x_minus(self, tiles, t):
        n = len(tiles)
        last = self.lane >= LANES - self.nz
        both = tiles[t] if n == 1 else jnp.where(last, tiles[(t - 1) % n], tiles[t])
        return pltpu.roll(both, self.nz, 1)

    def y_plus(self, tile, following):
        return pltpu.roll(jnp.where(self.row == 0, following, tile), SUB - 1, 0)

    def y_minus(self, tile, previous):
        return pltpu.roll(jnp.where(self.row == SUB - 1, previous, tile), 1, 0)

    def z_plus(self, tile):
        return jnp.where(self.not_top, pltpu.roll(tile, LANES - 1, 1), 0.0)

    def z_minus(self, tile):
        return jnp.where(self.not_bottom, pltpu.roll(tile, 1, 1), 0.0)


def tile_of(t):
    return slice(t * LANES, (t + 1) * LANES)


def row_loop(tiles, unroll, body):
    while tiles % unroll:
        unroll -= 1

    def step(i, carry):
        for k in range(unroll):
            body(pl.multiple_of((i * unroll + k) * SUB, SUB))
        return carry

    lax.fori_loop(0, tiles // unroll, step, 0)


class Packed:
    def __init__(self, level, nz, n):
        self.n = n
        self.half = half = nz // 2
        self.scale = scale = 1.0 / float(4**level)
        lane, row = iota2((SUB, LANES), 1), iota2((SUB, LANES), 0)
        zh = lane % half
        diag_in, diag_edge = HELMHOLTZ + 6.0 * scale, HELMHOLTZ + 5.0 * scale
        odd = ((lane // half) * n + row) % 2 == 1
        self.odd = [odd, ~odd]
        self.up, self.down, self.diag, self.inv, self.take = [], [], [], [], []
        for v in (0, 1):
            up = self.odd[v] & (zh < half - 1)
            down = self.odd[1 - v] & (zh > 0)
            inside = up | down
            self.up.append(up)
            self.down.append(down)
            self.diag.append(jnp.where(inside, diag_in, diag_edge).astype(jnp.float32))
            self.inv.append(jnp.where(inside, 1.0 / diag_in, 1.0 / diag_edge).astype(jnp.float32))
            self.take.append(jnp.where(inside, scale / diag_in, scale / diag_edge).astype(jnp.float32))

    def totals(self, q, other, r):
        n = self.n
        here = [q[other, k, pl.ds(r, SUB), :] for k in range(n)]
        first = pltpu.roll(here[0], LANES - self.half, 1)
        last = pltpu.roll(here[n - 1], self.half, 1)
        out = []
        for k in range(n):
            v = (k + 1 - other) % 2
            b = here[k]
            east = here[k + 1] if k < n - 1 else first
            west = here[k - 1] if k > 0 else last
            north = q[other, k, pl.ds(r + 1, SUB), :]
            south = q[other, k, pl.ds(r - 1, SUB), :]
            z = jnp.where(
                self.up[v],
                pltpu.roll(b, LANES - 1, 1),
                jnp.where(self.down[v], pltpu.roll(b, 1, 1), 0.0),
            )
            out.append((east + west) + (north + south) + (b + z))
        return out

    def first(self, q, f, start, count, unroll):
        def body(i):
            for k in range(self.n):
                r = i + start
                q[0, k, pl.ds(r + SUB, SUB), :] = f[0, k, pl.ds(r, SUB), :] * self.inv[k % 2]

        row_loop(count, unroll, body)

    def half_sweep(self, q, f, c, start, count, unroll, wrap):
        if wrap:
            wrap_rows(q, 1 - c)

        def body(i):
            r = i + start
            total = self.totals(q, 1 - c, r + SUB)
            for k in range(self.n):
                v = (k + c) % 2
                q[c, k, pl.ds(r + SUB, SUB), :] = (
                    f[c, k, pl.ds(r, SUB), :] * self.inv[v] + total[k] * self.take[v]
                )

        row_loop(count, unroll, body)

    def presmooth(self, q, f, sweeps, count, unroll, wrap):
        self.first(q, f, 0, count, unroll)
        for k in range(1, 2 * sweeps):
            self.half_sweep(q, f, k % 2, 0, count, unroll, wrap)

    def postsmooth(self, q, f, start, count, unroll, wrap):
        for k in range(2 * SWEEPS):
            self.half_sweep(q, f, k % 2, start, count, unroll, wrap)

    def residual(self, q, f, out, start, count, unroll, wrap):
        if wrap:
            wrap_rows(q, 0)
            wrap_rows(q, 1)
        n = self.n

        def body(i):
            r = i + start
            parts = [None] * n
            for c in (0, 1):
                total = self.totals(q, 1 - c, r + SUB)
                for k in range(n):
                    v = (k + c) % 2
                    res = f[c, k, pl.ds(r, SUB), :] - (
                        self.diag[v] * q[c, k, pl.ds(r + SUB, SUB), :] - self.scale * total[k]
                    )
                    parts[k] = res if c == 0 else parts[k] + res
            if n == 1:
                out[0, pl.ds(i, SUB), :] = parts[0]
            else:
                for j in range(n // 2):
                    out[j, pl.ds(i, SUB), :] = parts[2 * j] + parts[2 * j + 1]

        row_loop(count, unroll, body)

    def colours(self, even, odd, k):
        rows = even.shape[0]
        odd_cell = jnp.concatenate([self.odd[k % 2]] * (rows // SUB), axis=0)
        return jnp.where(odd_cell, odd, even), jnp.where(odd_cell, even, odd)


def wrap_rows(q, c):
    rows = q.shape[2]
    for k in range(q.shape[1]):
        q[c, k, 0:SUB, :] = q[c, k, rows - 2 * SUB : rows - SUB, :]
        q[c, k, rows - SUB : rows, :] = q[c, k, SUB : 2 * SUB, :]


def pair_rows(ref, j, rows):
    return ref[j, pl.ds(0, rows, stride=2), :] + ref[j, pl.ds(1, rows, stride=2), :]


def twice_rows(value, pairs, j):
    rows = value.shape[0]
    pairs[j, pl.ds(0, rows, stride=2), :] = value
    pairs[j, pl.ds(1, rows, stride=2), :] = value


def matrix(rows, cols, weight, hit):
    i, o = iota2((rows, cols), 0), iota2((rows, cols), 1)
    return jnp.where(hit(i, o), weight, 0.0).astype(jnp.float32)


def kernel(
    nx_dev, ny_dev, nz, nx, ny,
    vel_in, old_in, obs_in, cor_out, pre_out,
    vel, old, fluid, edge, edge_in, pred,
    f0, fn, hn, f0q, p0, cs, cr, gath, f1, p1, m2, f2, p2, f3, p3, pairs,
    predn, pn, gn, send_sem, recv_sem,
):
    gx, gy = lax.axis_index("gx"), lax.axis_index("gy")

    def device(dx, dy):
        return (lax.rem(gx + dx + nx_dev, nx_dev), lax.rem(gy + dy + ny_dev, ny_dev))

    peers = [(d, 0) for d in range(1, nx_dev)] + [(0, d) for d in range(1, ny_dev)]
    peers += [(a, b) for a in range(1, nx_dev) for b in (-1, 1)]
    barrier = pltpu.get_barrier_semaphore()
    for dx, dy in peers:
        pl.semaphore_signal(barrier, inc=1, device_id=device(dx, dy), device_id_type=MESH)

    number = [0]

    def send(src, dst, dx, dy):
        k = number[0]
        number[0] += 1
        copy = pltpu.make_async_remote_copy(
            src_ref=src, dst_ref=dst, send_sem=send_sem.at[k], recv_sem=recv_sem.at[k],
            device_id=device(dx, dy), device_id_type=MESH,
        )
        copy.start()
        return copy

    per = LANES // nz
    blocks = nx // per
    width = blocks * LANES
    lv0 = Level(0, nz)
    lane = lv0.lane

    def load_tile(ref, base, t):
        rows = [ref[pl.ds(base + t * per + i, nz, stride=nx), :] for i in range(per)]
        return jnp.concatenate(rows, axis=0).T

    for c in range(3):
        for t in range(blocks):
            vel[c, SUB : SUB + ny, tile_of(t + 1)] = load_tile(vel_in, c * nz * nx, t)

    pltpu_wait = functools.partial(pl.semaphore_wait, barrier)
    pltpu_wait(len(peers))

    def join(high):
        parts = []
        for c in range(3):
            source = vel[c, SUB : SUB + ny, tile_of(blocks if high else 1)]
            start = LANES - nz if high else 0
            parts.append(pltpu.roll(source, (c * nz - start) % LANES, 1))
        wide = iota2((ny, LANES), 1)
        return jnp.where(wide < nz, parts[0], jnp.where(wide < 2 * nz, parts[1], parts[2]))

    copies = [
        send(vel.at[:, ny : ny + SUB, LANES : LANES + width], vel.at[:, 0:SUB, LANES : LANES + width], 0, 1),
        send(
            vel.at[:, SUB : 2 * SUB, LANES : LANES + width],
            vel.at[:, SUB + ny : 2 * SUB + ny, LANES : LANES + width], 0, -1,
        ),
    ]
    edge[0] = join(True)
    copies.append(send(edge.at[0], edge_in.at[0], 1, 0))
    edge[1] = join(False)
    copies.append(send(edge.at[1], edge_in.at[1], -1, 0))

    for c in range(3):
        for t in range(blocks):
            old[c, :, tile_of(t)] = load_tile(old_in, c * nz * nx, t)
    for t in range(blocks):
        fluid[:, tile_of(t)] = (1 - load_tile(obs_in, 0, t)).astype(jnp.float32)
    for copy in copies:
        copy.wait()
    for c in range(3):
        vel[c, SUB : SUB + ny, tile_of(0)] = pltpu.roll(edge_in[0], (LANES - nz - c * nz) % LANES, 1)
        vel[c, SUB : SUB + ny, tile_of(blocks + 1)] = pltpu.roll(edge_in[1], (-c * nz) % LANES, 1)

    def momentum(r):
        here = [
            [vel[c, pl.ds(r + SUB, SUB), tile_of(t)] for t in range(blocks + 2)] for c in range(3)
        ]
        for t in range(1, blocks + 1):
            cols = tile_of(t)
            wet = fluid[pl.ds(r, SUB), tile_of(t - 1)]
            for c in range(3):
                q = here[c][t]
                xp, xm = lv0.x_plus(here[c], t), lv0.x_minus(here[c], t)
                yp = lv0.y_plus(q, vel[c, pl.ds(r + 2 * SUB, SUB), cols])
                ym = lv0.y_minus(q, vel[c, pl.ds(r, SUB), cols])
                zp, zm = lv0.z_plus(q), lv0.z_minus(q)
                advect = 0.5 * (
                    here[0][t] * (xp - xm) + here[1][t] * (yp - ym) + here[2][t] * (zp - zm)
                )
                diffuse = xp + xm + yp + ym + zp + zm - 6.0 * q
                tendency = VISCOSITY * diffuse - advect
                pred[c, pl.ds(r + SUB, SUB), cols] = wet * (
                    q
                    + TIME_STEP
                    * (WEIGHT_NEW * tendency + WEIGHT_OLD * old[c, pl.ds(r, SUB), tile_of(t - 1)])
                )

    row_loop(ny // SUB, 2, momentum)

    inner = slice(LANES, LANES + width)
    copies = [
        send(pred.at[0, SUB : SUB + ny, tile_of(blocks)], pred.at[0, SUB : SUB + ny, tile_of(0)], 1, 0),
        send(pred.at[0, SUB : SUB + ny, tile_of(1)], pred.at[0, SUB : SUB + ny, tile_of(blocks + 1)], -1, 0),
        send(pred.at[1, ny : ny + SUB, inner], pred.at[1, 0:SUB, inner], 0, 1),
        send(pred.at[1, SUB : 2 * SUB, inner], pred.at[1, SUB + ny : 2 * SUB + ny, inner], 0, -1),
    ]
    for copy in copies:
        copy.wait()

    side = HALO_X // per

    def divergence(r):
        u = [pred[0, pl.ds(r + SUB, SUB), tile_of(t)] for t in range(blocks + 2)]
        for t in range(1, blocks + 1):
            cols = tile_of(t)
            v = pred[1, pl.ds(r + SUB, SUB), cols]
            w = pred[2, pl.ds(r + SUB, SUB), cols]
            v_plus = lv0.y_plus(v, pred[1, pl.ds(r + 2 * SUB, SUB), cols])
            v_minus = lv0.y_minus(v, pred[1, pl.ds(r, SUB), cols])
            total = (
                (lv0.x_plus(u, t) - lv0.x_minus(u, t))
                + (v_plus - v_minus)
                + (lv0.z_plus(w) - lv0.z_minus(w))
            )
            f0[pl.ds(r, SUB), tile_of(t - 1)] = total * (-0.5 / TIME_STEP)

    row_loop(ny // SUB, 2, divergence)

    for t in range(blocks):
        fn[t] = f0[:, tile_of(t)].T
    copies = [
        send(fn.at[blocks - side : blocks], hn.at[0:side], 1, 0),
        send(fn.at[0:side], hn.at[side : 2 * side], -1, 0),
    ]

    n0, half0 = per, nz // 2
    lv0p = Packed(0, nz, n0)
    tall0 = ny + 2 * HALO_Y
    blank = jnp.zeros((half0, ny), jnp.float32)
    spare = LANES // half0 - blocks - 2 * side

    def pack(k, e, whole):
        pick = pl.ds(k * nz + e, half0, stride=2)
        rows = []
        for j in range(side):
            rows.append(hn[j, pick, :] if whole else blank)
        for t in range(blocks):
            rows.append(fn[t, pick, :])
        for j in range(side):
            rows.append(hn[side + j, pick, :] if whole else blank)
        rows += [blank] * spare
        return jnp.concatenate(rows, axis=0).T

    def own_pack(whole):
        for k in range(n0):
            both = lv0p.colours(pack(k, 0, whole), pack(k, 1, whole), k)
            for c in (0, 1):
                f0q[c, k, HALO_Y : HALO_Y + ny, :] = both[c]

    own_pack(False)
    edges = {1: slice(ny, ny + HALO_Y), -1: slice(HALO_Y, 2 * HALO_Y)}
    ends = {1: slice(0, HALO_Y), -1: slice(ny + HALO_Y, ny + 2 * HALO_Y)}
    group = iota2((SUB, LANES), 1) // half0
    slots = LANES // half0
    corners = [(a, b) for a in (1, -1) for b in (1, -1)]
    for i, (dx, dy) in enumerate(corners):
        for j in range(side):
            own = (blocks if dx > 0 else side) + j
            out = None
            for m in range(2 * n0):
                value = f0q[m // n0, m % n0, edges[dy], :]
                value = pltpu.roll(value, ((m - own) * half0) % LANES, 1)
                out = value if out is None else jnp.where(group == m, value, out)
            cs[i, j] = out
    for dy in (1, -1):
        copies.append(send(f0q.at[:, :, edges[dy], :], cr.at[4 + (dy < 0)], 0, dy))
    for i, (dx, dy) in enumerate(corners):
        copies.append(send(cs.at[i], cr.at[i, 0, 0:side], dx, dy))

    def turn_rows(ref, base, t, turned):
        for i in range(per):
            ref[pl.ds(base + t * per + i, nz, stride=nx), :] = turned[i * nz : (i + 1) * nz, :]

    for c in range(3):
        for t in range(blocks):
            turn_rows(predn, c * nz * nx, t, pred[c, SUB : SUB + ny, tile_of(t + 1)].T)

    p0[...] = jnp.zeros(p0.shape, jnp.float32)
    p1[...] = jnp.zeros(p1.shape, jnp.float32)
    for copy in copies:
        copy.wait()

    own_pack(True)
    for dy in (1, -1):
        for m in range(2 * n0):
            value = cr[4 + (dy < 0), m // n0, m % n0]
            for i, (dx, cy) in enumerate(corners):
                if cy == dy:
                    for j in range(side):
                        g = j if dx > 0 else side + blocks + j
                        part = pltpu.roll(cr[i, 0, j], ((g - m) * half0) % LANES, 1)
                        value = jnp.where(group == g, part, value)
            f0q[m // n0, m % n0, ends[dy], :] = value

    tiles0 = tall0 // SUB
    lv0p.presmooth(p0, f0q, SWEEPS, tiles0, tiles0, False)
    lv0p.residual(p0, f0q, pairs, HALO_Y, ny // SUB, ny // SUB, False)

    own_x, nz1, half1 = nx // 2, nz // 2, nz // 4
    n1 = nx_dev * own_x * half1 // LANES
    lv1 = Packed(1, nz1, n1)
    wide = own_x // n1 * half1
    rows1 = ny // 2

    def down0(i, o):
        x = 2 * ((i % LANES) // half0 - side) + i // LANES
        z = i % half0
        place = ((z % 2) * n1 + x % n1) * wide + (x // n1) * half1 + z // 2
        return (x >= 0) & (x < own_x) & (place == o)

    sums = jnp.concatenate([pair_rows(pairs, j, rows1) for j in range(n0 // 2)], axis=1)
    gath[0, HALO_1 : HALO_1 + rows1, :] = mm(sums, matrix(LANES * (n0 // 2), LANES, 0.125, down0))
    body1 = slice(HALO_1, HALO_1 + rows1)
    copies = [send(gath.at[0, body1], gath.at[j, body1], nx_dev - j, 0) for j in range(1, nx_dev)]
    for j in range(nx_dev):
        copies.append(send(gath.at[0, rows1 : rows1 + HALO_1], gath.at[j, 0:HALO_1], nx_dev - j, 1))
        copies.append(
            send(gath.at[0, HALO_1 : 2 * HALO_1], gath.at[j, rows1 + HALO_1 : rows1 + 2 * HALO_1], nx_dev - j, -1)
        )
    for copy in copies:
        copy.wait()

    tall1 = rows1 + 2 * HALO_1
    source = iota2((SUB, LANES), 1) // wide

    def spread(r):
        parts = [gath[j, pl.ds(r, SUB), :] for j in range(nx_dev)]
        arr = []
        for m in range(2 * n1):
            out = pltpu.roll(parts[0], (-m * wide) % LANES, 1) if m else parts[0]
            for j in range(1, nx_dev):
                moved = pltpu.roll(parts[j], ((j - m) * wide) % LANES, 1) if j != m else parts[j]
                out = jnp.where(source == j, moved, out)
            arr.append(out)
        for k in range(n1):
            both = lv1.colours(arr[k], arr[n1 + k], k)
            f1[0, k, pl.ds(r, SUB), :] = both[0]
            f1[1, k, pl.ds(r, SUB), :] = both[1]

    tiles1 = tall1 // SUB
    row_loop(tiles1, tiles1, spread)
    lv1.presmooth(p1, f1, SWEEPS, tiles1, tiles1, False)
    lv1.residual(p1, f1, pairs, HALO_1, rows1 // SUB, rows1 // SUB, False)

    x2, nz2, half2 = nx_dev * nx // 4, nz // 4, nz // 8
    lanes2 = x2 * half2
    lv2 = Packed(2, nz2, 1)
    pieces = max(1, n1 // 2)
    own2 = ny // 4

    def down1(i, o):
        x = (i % LANES) // half1 * pieces + i // LANES
        z = i % half1
        return (z % 2) * lanes2 + x * half2 + z // 2 == o

    sums = jnp.concatenate([pair_rows(pairs, j, own2) for j in range(pieces)], axis=1)
    m2[0:own2, :] = mm(sums, matrix(LANES * pieces, 2 * lanes2, 0.125, down1))
    copies = [
        send(m2.at[0:own2, :], m2.at[j * own2 : (j + 1) * own2, :], 0, ny_dev - j) for j in range(1, ny_dev)
    ]
    for copy in copies:
        copy.wait()
    rows2 = ny_dev * own2
    low_half = iota2((SUB, LANES), 1) < LANES // 2

    def spread2(r):
        if lanes2 == LANES:
            even, odd = m2[pl.ds(r, SUB), 0:LANES], m2[pl.ds(r, SUB), LANES : 2 * LANES]
        else:
            both = m2[pl.ds(r, SUB), :]
            turned = pltpu.roll(both, LANES // 2, 1)
            even, odd = jnp.where(low_half, both, turned), jnp.where(low_half, turned, both)
        both = lv2.colours(even, odd, 0)
        f2[0, 0, pl.ds(r, SUB), :] = both[0]
        f2[1, 0, pl.ds(r, SUB), :] = both[1]

    row_loop(rows2 // SUB, 32, spread2)
    lv2.presmooth(p2, f2, SWEEPS, rows2 // SUB, 32, True)
    lv2.residual(p2, f2, pairs, 0, rows2 // SUB, 32, True)

    x3, half3 = x2 // 2, half2 // 2
    lv3 = Packed(3, nz2 // 2, 1)
    rows3 = rows2 // 2

    def down2(i, o):
        lane = o % LANES
        hit = (i < lanes2) & (i // half2 // 2 == (lane // half3) % x3)
        return hit & (i % half2 == 2 * (lane % half3) + o // LANES)

    down = mm(pair_rows(pairs, 0, rows3), matrix(LANES, 2 * LANES, 0.125, down2))
    both = lv3.colours(down[:, 0:LANES], down[:, LANES : 2 * LANES], 0)
    f3[0, 0] = both[0]
    f3[1, 0] = both[1]
    lv3.presmooth(p3, f3, COARSE_SWEEPS, rows3 // SUB, 16, True)

    def up3(i, o):
        lane = i % LANES
        hit = (lane < x3 * half3) & (lane // half3 == (o // half2) % x2 // 2)
        return hit & (2 * (lane % half3) + i // LANES == o % half2)

    inner3 = slice(SUB, SUB + rows3)
    both = lv3.colours(p3[0, 0, inner3, :], p3[1, 0, inner3, :], 0)
    twice_rows(mm(jnp.concatenate(both, axis=1), matrix(2 * LANES, LANES, 1.0, up3)), pairs, 0)
    p2[1, 0, SUB : SUB + rows2, :] += pairs[0, 0:rows2, :]
    lv2.postsmooth(p2, f2, 0, rows2 // SUB, 32, True)
    wrap_rows(p2, 0)
    wrap_rows(p2, 1)

    def up2(i, o):
        lane, to = i % LANES, o % LANES
        hit = (lane < lanes2) & (lane // half2 == (to // half1) * pieces + o // LANES)
        return hit & (2 * (lane % half2) + i // LANES == to % half1)

    first2 = SUB - HALO_1 // 2
    window = slice(first2, first2 + tall1 // 2)
    both = lv2.colours(p2[0, 0, window, :], p2[1, 0, window, :], 0)
    lift = mm(jnp.concatenate(both, axis=1), matrix(2 * LANES, LANES * pieces, 1.0, up2))
    for j in range(pieces):
        twice_rows(lift[:, tile_of(j)], pairs, j)
    for k in range(n1):
        p1[1, k, SUB : SUB + tall1, :] += pairs[k * pieces // n1, 0:tall1, :]
    lv1.postsmooth(p1, f1, 0, tiles1, tiles1, False)

    reach = side * n0 // 2
    wide_x = own_x + 2 * reach
    take = wide_x // n1 * half1
    off = -reach // n1 * half1
    first1 = SUB + HALO_1 - HALO_Y // 2
    window = slice(first1, first1 + tall0 // 2)
    halves = [[], []]
    for k in range(n1):
        both = lv1.colours(p1[0, k, window, :], p1[1, k, window, :], k)
        halves[0].append(both[0])
        halves[1].append(both[1])
    slot = iota2((tall0 // 2, LANES), 1) // take
    joined = []
    for e in (0, 1):
        out = None
        for k in range(n1):
            moved = pltpu.roll(halves[e][k], (k * take - off) % LANES, 1)
            out = moved if out is None else jnp.where(slot == k, moved, out)
        joined.append(out)

    def up1(i, o):
        lane, to = i % LANES, o % LANES
        x = (lane % take) // half1 * n1 + lane // take
        hit = (lane < take * n1) & (x == to // half0 * (n0 // 2) + o // LANES)
        return hit & (2 * (lane % half1) + i // LANES == to % half0)

    lift = mm(jnp.concatenate(joined, axis=1), matrix(2 * LANES, LANES * (n0 // 2), 1.0, up1))
    for j in range(n0 // 2):
        twice_rows(lift[:, tile_of(j)], pairs, j)
    for k in range(n0):
        p0[1, k, SUB : SUB + tall0, :] += pairs[k // 2, 0:tall0, :]
    lv0p.postsmooth(p0, f0q, 0, tiles0, tiles0, False)

    low = SUB + HALO_Y
    body0 = slice(low, low + ny)
    ext = nx + 2 * HALO_X
    for k in range(n0):
        value = lv0p.colours(p0[0, k, body0, :], p0[1, k, body0, :], k)
        slope = [
            p0[1 - c, k, low + 1 : low + 1 + ny, :] - p0[1 - c, k, low - 1 : low - 1 + ny, :] for c in (0, 1)
        ]
        slope = lv0p.colours(slope[0], slope[1], k)
        for e in (0, 1):
            turned, sloped = value[e].T, slope[e].T
            for b in range(side - 1, side + blocks + 1):
                part = slice(b * half0, (b + 1) * half0)
                pn[pl.ds(e * ext + b * n0 + k, half0, stride=2 * ext), :] = turned[part, :]
                if side <= b < side + blocks:
                    gn[pl.ds(e * nx + (b - side) * n0 + k, half0, stride=2 * nx), :] = sloped[part, :]

    def correct(z):
        for h in range(nx // SUB):
            def cells(dz, dx):
                return pn[pl.ds((z + dz) * ext + HALO_X + h * SUB + dx, SUB), :]

            here = pl.ds(z * nx + h * SUB, SUB)
            pre_out[here, :] = cells(0, 0)
            wet = (1 - obs_in[here, :]).astype(jnp.float32)
            above = cells(1, 0) if z < nz - 1 else 0.0
            below = cells(-1, 0) if z > 0 else 0.0
            slope = (cells(0, 1) - cells(0, -1), gn[here, :], above - below)
            for c in range(3):
                there = pl.ds(c * nz * nx + z * nx + h * SUB, SUB)
                cor_out[there, :] = wet * (predn[there, :] - (0.5 * TIME_STEP) * slope[c])

    for z in range(nz):
        correct(z)


def body(nx_dev, ny_dev, velocity, old_tendency, obstacle):
    _, nz, nx, ny = velocity.shape
    width = nx * nz
    per = LANES // nz
    blocks = nx // per
    side = HALO_X // per
    tall0 = ny + 2 * HALO_Y
    n1 = nx_dev * (nx // 2) * (nz // 4) // LANES
    tall1 = ny // 2 + 2 * HALO_1
    rows2 = ny_dev * ny // 4
    rows3 = rows2 // 2
    wide2 = 2 * (nx_dev * nx // 4) * (nz // 8)
    tall = max(tall0, tall1, rows2)
    count = max(per // 2, n1 // 2, 1)
    copies = 4 + 4 + 2 + 2 + 4 + (nx_dev - 1) + 2 * nx_dev + (ny_dev - 1)
    f32 = jnp.float32
    out = pl.pallas_call(
        functools.partial(kernel, nx_dev, ny_dev, nz, nx, ny),
        out_shape=(
            jax.ShapeDtypeStruct((3 * nz * nx, ny), f32),
            jax.ShapeDtypeStruct((nz * nx, ny), f32),
        ),
        in_specs=[pl.BlockSpec(memory_space=pltpu.VMEM)] * 3,
        out_specs=[pl.BlockSpec(memory_space=pltpu.VMEM)] * 2,
        scratch_shapes=[
            pltpu.VMEM((3, ny + 2 * SUB, width + 2 * LANES), f32),
            pltpu.VMEM((3, ny, width), f32),
            pltpu.VMEM((ny, width), f32),
            pltpu.VMEM((2, ny, LANES), f32),
            pltpu.VMEM((2, ny, LANES), f32),
            pltpu.VMEM((3, ny + 2 * SUB, width + 2 * LANES), f32),
            pltpu.VMEM((ny, width), f32),
            pltpu.VMEM((blocks, LANES, ny), f32),
            pltpu.VMEM((2 * side, LANES, ny), f32),
            pltpu.VMEM((2, per, tall0, LANES), f32),
            pltpu.VMEM((2, per, tall0 + 2 * SUB, LANES), f32),
            pltpu.VMEM((4, side, SUB, LANES), f32),
            pltpu.VMEM((6, 2, per, SUB, LANES), f32),
            pltpu.VMEM((nx_dev, tall1, LANES), f32),
            pltpu.VMEM((2, n1, tall1, LANES), f32),
            pltpu.VMEM((2, n1, tall1 + 2 * SUB, LANES), f32),
            pltpu.VMEM((rows2, wide2), f32),
            pltpu.VMEM((2, 1, rows2, LANES), f32),
            pltpu.VMEM((2, 1, rows2 + 2 * SUB, LANES), f32),
            pltpu.VMEM((2, 1, rows3, LANES), f32),
            pltpu.VMEM((2, 1, rows3 + 2 * SUB, LANES), f32),
            pltpu.VMEM((count, tall, LANES), f32),
            pltpu.VMEM((3 * nz * nx, ny), f32),
            pltpu.VMEM((nz * (nx + 2 * HALO_X), ny), f32),
            pltpu.VMEM((nz * nx, ny), f32),
            pltpu.SemaphoreType.DMA((copies,)),
            pltpu.SemaphoreType.DMA((copies,)),
        ],
        compiler_params=pltpu.CompilerParams(
            collective_id=0, has_side_effects=True, vmem_limit_bytes=60 * 1024 * 1024
        ),
    )(
        velocity.reshape(3 * nz * nx, ny),
        old_tendency.reshape(3 * nz * nx, ny),
        obstacle.reshape(nz * nx, ny),
    )
    return out[0].reshape(3, nz, nx, ny), out[1].reshape(nz, nx, ny)


def solution(mesh):
    placed = (P(None, None, "gx", "gy"), P(None, None, "gx", "gy"), P(None, "gx", "gy"))
    return jax.shard_map(
        functools.partial(body, mesh.shape["gx"], mesh.shape["gy"]),
        mesh=mesh,
        in_specs=placed,
        out_specs=(P(None, None, "gx", "gy"), P(None, "gx", "gy")),
        check_vma=False,
    )
```

```python
import functools

import jax
import jax.numpy as jnp
from jax import lax
from jax.experimental import pallas as pl
from jax.experimental.pallas import tpu as pltpu
from jax.sharding import PartitionSpec as P

LEVELS = 3
SWEEPS = 2
COARSE_SWEEPS = 8
VISCOSITY = 0.1
TIME_STEP = 0.25
WEIGHT_NEW = 15.0 / 16.0
WEIGHT_OLD = -25.0 / 48.0
HELMHOLTZ = 0.0001

LANES = 128
SUB = 8
HALO_X = 8
HALO_Y = 8
HALO_1 = 16
MESH = pl.DeviceIdType.MESH


def iota2(shape, dim):
    return lax.broadcasted_iota(jnp.int32, shape, dim)


def mm(a, b):
    return jnp.dot(a, b, precision=lax.Precision.HIGHEST, preferred_element_type=jnp.float32)


class Level:
    def __init__(self, level, nz):
        self.nz = nz
        self.scale = 1.0 / float(4**level)
        lane = iota2((SUB, LANES), 1)
        row = iota2((SUB, LANES), 0)
        self.lane = lane
        self.row = row
        z = lane % nz
        self.not_top = z < nz - 1
        self.not_bottom = z > 0
        parity = (z + lane // nz + row) % 2
        self.colour = [parity == 0, parity == 1]
        edge = (z == 0) | (z == nz - 1)
        diag_in = HELMHOLTZ + 6.0 * self.scale
        diag_edge = HELMHOLTZ + 5.0 * self.scale
        self.diag = jnp.where(edge, diag_edge, diag_in).astype(jnp.float32)
        self.inv = jnp.where(edge, 1.0 / diag_edge, 1.0 / diag_in).astype(jnp.float32)
        self.take = jnp.where(
            edge, self.scale / diag_edge, self.scale / diag_in
        ).astype(jnp.float32)

    def x_plus(self, tiles, t):
        n = len(tiles)
        both = tiles[t] if n == 1 else jnp.where(self.lane < self.nz, tiles[(t + 1) % n], tiles[t])
        return pltpu.roll(both, LANES - self.nz, 1)

    def x_minus(self, tiles, t):
        n = len(tiles)
        last = self.lane >= LANES - self.nz
        both = tiles[t] if n == 1 else jnp.where(last, tiles[(t - 1) % n], tiles[t])
        return pltpu.roll(both, self.nz, 1)

    def y_plus(self, tile, following):
        return pltpu.roll(jnp.where(self.row == 0, following, tile), SUB - 1, 0)

    def y_minus(self, tile, previous):
        return pltpu.roll(jnp.where(self.row == SUB - 1, previous, tile), 1, 0)

    def z_plus(self, tile):
        return jnp.where(self.not_top, pltpu.roll(tile, LANES - 1, 1), 0.0)

    def z_minus(self, tile):
        return jnp.where(self.not_bottom, pltpu.roll(tile, 1, 1), 0.0)


def tile_of(t):
    return slice(t * LANES, (t + 1) * LANES)


def row_loop(tiles, unroll, body):
    while tiles % unroll:
        unroll -= 1

    def step(i, carry):
        for k in range(unroll):
            body(pl.multiple_of((i * unroll + k) * SUB, SUB))
        return carry

    lax.fori_loop(0, tiles // unroll, step, 0)


class Packed:
    def __init__(self, level, nz, n):
        self.n = n
        self.half = half = nz // 2
        self.scale = scale = 1.0 / float(4**level)
        lane, row = iota2((SUB, LANES), 1), iota2((SUB, LANES), 0)
        zh = lane % half
        diag_in, diag_edge = HELMHOLTZ + 6.0 * scale, HELMHOLTZ + 5.0 * scale
        odd = ((lane // half) * n + row) % 2 == 1
        self.odd = [odd, ~odd]
        self.up, self.down, self.diag, self.inv, self.take = [], [], [], [], []
        for v in (0, 1):
            up = self.odd[v] & (zh < half - 1)
            down = self.odd[1 - v] & (zh > 0)
            inside = up | down
            self.up.append(up)
            self.down.append(down)
            self.diag.append(jnp.where(inside, diag_in, diag_edge).astype(jnp.float32))
            self.inv.append(jnp.where(inside, 1.0 / diag_in, 1.0 / diag_edge).astype(jnp.float32))
            self.take.append(jnp.where(inside, scale / diag_in, scale / diag_edge).astype(jnp.float32))

    def totals(self, q, other, r):
        n = self.n
        here = [q[other, k, pl.ds(r, SUB), :] for k in range(n)]
        first = pltpu.roll(here[0], LANES - self.half, 1)
        last = pltpu.roll(here[n - 1], self.half, 1)
        out = []
        for k in range(n):
            v = (k + 1 - other) % 2
            b = here[k]
            east = here[k + 1] if k < n - 1 else first
            west = here[k - 1] if k > 0 else last
            north = q[other, k, pl.ds(r + 1, SUB), :]
            south = q[other, k, pl.ds(r - 1, SUB), :]
            z = jnp.where(
                self.up[v],
                pltpu.roll(b, LANES - 1, 1),
                jnp.where(self.down[v], pltpu.roll(b, 1, 1), 0.0),
            )
            out.append((east + west) + (north + south) + (b + z))
        return out

    def first(self, q, f, start, count, unroll):
        def body(i):
            for k in range(self.n):
                r = i + start
                q[0, k, pl.ds(r + SUB, SUB), :] = f[0, k, pl.ds(r, SUB), :] * self.inv[k % 2]

        row_loop(count, unroll, body)

    def half_sweep(self, q, f, c, start, count, unroll, wrap):
        if wrap:
            wrap_rows(q, 1 - c)

        def body(i):
            r = i + start
            total = self.totals(q, 1 - c, r + SUB)
            for k in range(self.n):
                v = (k + c) % 2
                q[c, k, pl.ds(r + SUB, SUB), :] = (
                    f[c, k, pl.ds(r, SUB), :] * self.inv[v] + total[k] * self.take[v]
                )

        row_loop(count, unroll, body)

    def presmooth(self, q, f, sweeps, count, unroll, wrap):
        self.first(q, f, 0, count, unroll)
        for k in range(1, 2 * sweeps):
            self.half_sweep(q, f, k % 2, 0, count, unroll, wrap)

    def postsmooth(self, q, f, start, count, unroll, wrap):
        for k in range(2 * SWEEPS):
            self.half_sweep(q, f, k % 2, start, count, unroll, wrap)

    def residual(self, q, f, out, start, count, unroll, wrap):
        if wrap:
            wrap_rows(q, 0)
            wrap_rows(q, 1)
        n = self.n

        def body(i):
            r = i + start
            parts = [None] * n
            for c in (0, 1):
                total = self.totals(q, 1 - c, r + SUB)
                for k in range(n):
                    v = (k + c) % 2
                    res = f[c, k, pl.ds(r, SUB), :] - (
                        self.diag[v] * q[c, k, pl.ds(r + SUB, SUB), :] - self.scale * total[k]
                    )
                    parts[k] = res if c == 0 else parts[k] + res
            if n == 1:
                out[0, pl.ds(i, SUB), :] = parts[0]
            else:
                for j in range(n // 2):
                    out[j, pl.ds(i, SUB), :] = parts[2 * j] + parts[2 * j + 1]

        row_loop(count, unroll, body)

    def colours(self, even, odd, k):
        rows = even.shape[0]
        odd_cell = jnp.concatenate([self.odd[k % 2]] * (rows // SUB), axis=0)
        return jnp.where(odd_cell, odd, even), jnp.where(odd_cell, even, odd)


def wrap_rows(q, c):
    rows = q.shape[2]
    for k in range(q.shape[1]):
        q[c, k, 0:SUB, :] = q[c, k, rows - 2 * SUB : rows - SUB, :]
        q[c, k, rows - SUB : rows, :] = q[c, k, SUB : 2 * SUB, :]


def pair_rows(ref, j, rows):
    return ref[j, pl.ds(0, rows, stride=2), :] + ref[j, pl.ds(1, rows, stride=2), :]


def twice_rows(value, pairs, j):
    rows = value.shape[0]
    pairs[j, pl.ds(0, rows, stride=2), :] = value
    pairs[j, pl.ds(1, rows, stride=2), :] = value


def matrix(rows, cols, weight, hit):
    i, o = iota2((rows, cols), 0), iota2((rows, cols), 1)
    return jnp.where(hit(i, o), weight, 0.0).astype(jnp.float32)


def kernel(
    nx_dev, ny_dev, nz, nx, ny,
    vel_in, old_in, obs_in, cor_out, pre_out,
    vel, old, fluid, edge, edge_in, pred,
    fe, fe_in, pe, pe_in, f0, fn, fs, f0q, p0, pk, pk_in, py_in,
    gath, f1, p1, m2, f2, p2, f3, p3, pairs, predn, pn, gn, send_sem, recv_sem,
):
    gx, gy = lax.axis_index("gx"), lax.axis_index("gy")

    def device(dx, dy):
        return (lax.rem(gx + dx + nx_dev, nx_dev), lax.rem(gy + dy + ny_dev, ny_dev))

    peers = [(d, 0) for d in range(1, nx_dev)] + [(0, d) for d in range(1, ny_dev)]
    peers += [(a, b) for a in range(1, nx_dev) for b in (-1, 1)]
    barrier = pltpu.get_barrier_semaphore()
    for dx, dy in peers:
        pl.semaphore_signal(barrier, inc=1, device_id=device(dx, dy), device_id_type=MESH)

    number = [0]

    def send(src, dst, dx, dy):
        k = number[0]
        number[0] += 1
        copy = pltpu.make_async_remote_copy(
            src_ref=src, dst_ref=dst, send_sem=send_sem.at[k], recv_sem=recv_sem.at[k],
            device_id=device(dx, dy), device_id_type=MESH,
        )
        copy.start()
        return copy

    per = LANES // nz
    blocks = nx // per
    width = blocks * LANES
    lv0 = Level(0, nz)
    lane = lv0.lane

    def load_tile(ref, base, t):
        rows = [ref[pl.ds(base + t * per + i, nz, stride=nx), :] for i in range(per)]
        return jnp.concatenate(rows, axis=0).T

    for i in (0, 1):
        for c in range(3):
            edge[i, c * nz : (c + 1) * nz, :] = vel_in[
                pl.ds(c * nz * nx + (nx - 1 if i == 0 else 0), nz, stride=nx), :
            ]
    for c in range(3):
        for t in range(blocks):
            vel[c, SUB : SUB + ny, tile_of(t + 1)] = load_tile(vel_in, c * nz * nx, t)

    pltpu_wait = functools.partial(pl.semaphore_wait, barrier)
    pltpu_wait(len(peers))

    copies = [
        send(edge.at[0], edge_in.at[0], 1, 0),
        send(edge.at[1], edge_in.at[1], -1, 0),
        send(vel.at[:, ny : ny + SUB, LANES : LANES + width], vel.at[:, 0:SUB, LANES : LANES + width], 0, 1),
        send(
            vel.at[:, SUB : 2 * SUB, LANES : LANES + width],
            vel.at[:, SUB + ny : 2 * SUB + ny, LANES : LANES + width], 0, -1,
        ),
    ]

    for c in range(3):
        for t in range(blocks):
            old[c, :, tile_of(t)] = load_tile(old_in, c * nz * nx, t)
    for t in range(blocks):
        fluid[:, tile_of(t)] = (1 - load_tile(obs_in, 0, t)).astype(jnp.float32)
    for copy in copies:
        copy.wait()
    rest = jnp.zeros((LANES - 3 * nz, ny), jnp.float32)
    beside = [jnp.concatenate([edge_in[i], rest], axis=0).T for i in (0, 1)]
    for c in range(3):
        vel[c, SUB : SUB + ny, tile_of(0)] = pltpu.roll(beside[0], (LANES - nz - c * nz) % LANES, 1)
        vel[c, SUB : SUB + ny, tile_of(blocks + 1)] = pltpu.roll(beside[1], (-c * nz) % LANES, 1)

    def momentum(r):
        here = [
            [vel[c, pl.ds(r + SUB, SUB), tile_of(t)] for t in range(blocks + 2)] for c in range(3)
        ]
        for t in range(1, blocks + 1):
            cols = tile_of(t)
            wet = fluid[pl.ds(r, SUB), tile_of(t - 1)]
            for c in range(3):
                q = here[c][t]
                xp, xm = lv0.x_plus(here[c], t), lv0.x_minus(here[c], t)
                yp = lv0.y_plus(q, vel[c, pl.ds(r + 2 * SUB, SUB), cols])
                ym = lv0.y_minus(q, vel[c, pl.ds(r, SUB), cols])
                zp, zm = lv0.z_plus(q), lv0.z_minus(q)
                advect = 0.5 * (
                    here[0][t] * (xp - xm) + here[1][t] * (yp - ym) + here[2][t] * (zp - zm)
                )
                diffuse = xp + xm + yp + ym + zp + zm - 6.0 * q
                tendency = VISCOSITY * diffuse - advect
                pred[c, pl.ds(r + SUB, SUB), cols] = wet * (
                    q
                    + TIME_STEP
                    * (WEIGHT_NEW * tendency + WEIGHT_OLD * old[c, pl.ds(r, SUB), tile_of(t - 1)])
                )

    row_loop(ny // SUB, 2, momentum)

    inner = slice(LANES, LANES + width)
    own_rows = slice(SUB, SUB + ny)
    factor = 0.5 / TIME_STEP
    side = HALO_X // per
    none = jnp.zeros((SUB, LANES), jnp.float32)

    def source_of(r, t, whole):
        cols = tile_of(t)
        rows = pl.ds(r, SUB)
        first, last = r == (0 if whole else SUB), r == (SUB + ny if whole else ny)
        u = [pred[0, rows, tile_of(i)] for i in range(blocks + 2)] if whole else (
            [none] + [pred[0, rows, tile_of(i)] for i in range(1, blocks + 1)] + [none]
        )
        v, w = pred[1, rows, cols], pred[2, rows, cols]
        north = none if last else pred[1, pl.ds(r + SUB, SUB), cols]
        south = none if first else pred[1, pl.ds(r - SUB, SUB), cols]
        total = (
            (lv0.x_plus(u, t) - lv0.x_minus(u, t))
            + (lv0.y_plus(v, north) - lv0.y_minus(v, south))
            + (lv0.z_plus(w) - lv0.z_minus(w))
        )
        return total * (-factor)

    def turn_rows(ref, base, t, turned):
        for i in range(per):
            ref[pl.ds(base + t * per + i, nz, stride=nx), :] = turned[i * nz : (i + 1) * nz, :]

    copies = [
        send(pred.at[:, ny : ny + SUB, inner], pred.at[:, 0:SUB, inner], 0, 1),
        send(pred.at[:, SUB : 2 * SUB, inner], pred.at[:, SUB + ny : 2 * SUB + ny, inner], 0, -1),
    ]
    for dx in (1, -1):
        i, t = (0, blocks) if dx > 0 else (1, 1)
        for r in range(0, ny, SUB):
            fe[i, r : r + SUB, :] = source_of(r + SUB, t, False)
        copies.append(send(fe.at[i], fe_in.at[i], dx, 0))
        turned = pred[0, own_rows, tile_of(t)].T
        pe[i] = turned[LANES - nz : LANES, :] if dx > 0 else turned[0:nz, :]
        copies.append(send(pe.at[i], pe_in.at[i], dx, 0))
        for dy in (1, -1):
            rows = slice(ny, ny + SUB) if dy > 0 else slice(SUB, 2 * SUB)
            there = slice(0, SUB) if dy > 0 else slice(SUB + ny, 2 * SUB + ny)
            copies.append(
                send(pred.at[:, rows, tile_of(t)], pred.at[:, there, tile_of(0 if dx > 0 else blocks + 1)], dx, dy)
            )
            copies.append(
                send(pred.at[1, rows, tile_of(t)], pred.at[1, rows, tile_of(0 if dx > 0 else blocks + 1)], dx, 0)
            )

    n0, half0 = per, nz // 2
    lv0p = Packed(0, nz, n0)
    tall0 = ny + 2 * HALO_Y
    blank = jnp.zeros((half0, ny), jnp.float32)
    group = iota2((SUB, LANES), 1) // half0
    slots = LANES // half0
    corners = [(a, b) for a in (1, -1) for b in (1, -1)]

    for c in range(3):
        for t in range(blocks):
            turn_rows(predn, c * nz * nx, t, pred[c, own_rows, tile_of(t + 1)].T)

    p0[...] = jnp.zeros(p0.shape, jnp.float32)
    p1[...] = jnp.zeros(p1.shape, jnp.float32)
    for copy in copies:
        copy.wait()

    blanks = jnp.zeros((LANES - nz, ny), jnp.float32)
    pred[0, own_rows, tile_of(0)] = jnp.concatenate([blanks, pe_in[0]], axis=0).T
    pred[0, own_rows, tile_of(blocks + 1)] = jnp.concatenate([pe_in[1], blanks], axis=0).T
    for r in range(0, tall0, SUB):
        strip = r == 0 or r == SUB + ny
        for t in range(blocks + 2):
            if strip or 1 <= t <= blocks:
                f0[r : r + SUB, tile_of(t)] = source_of(r, t, True)
                continue
            i = 0 if t == 0 else 1
            value = fe_in[i, r - SUB : r, :]
            near = pltpu.roll(
                pred[0, r : r + SUB, tile_of(1 if i == 0 else blocks)], LANES - nz if i == 0 else nz, 1
            )
            if i == 0:
                value = value - jnp.where(lane >= LANES - nz, factor * near, 0.0)
            else:
                value = value + jnp.where(lane < nz, factor * near, 0.0)
            if r == SUB:
                south = pltpu.roll(pred[1, 0:SUB, tile_of(t)], 1, 0)
                value = value + jnp.where(lv0.row == 0, factor * south, 0.0)
            if r == ny:
                north = pltpu.roll(pred[1, SUB + ny : 2 * SUB + ny, tile_of(t)], SUB - 1, 0)
                value = value - jnp.where(lv0.row == SUB - 1, factor * north, 0.0)
            f0[r : r + SUB, tile_of(t)] = value

    for t in range(blocks + 2):
        fn[t] = f0[own_rows, tile_of(t)].T
        strips = [f0[0:SUB, tile_of(t)], f0[SUB + ny : 2 * SUB + ny, tile_of(t)]]
        fs[t] = jnp.concatenate(strips + [jnp.zeros((LANES - 2 * SUB, LANES), jnp.float32)], axis=0).T

    def pack(ref, k, e):
        rows = [blank] * (side - 1)
        for t in range(blocks + 2):
            rows.append(ref[t, pl.ds(k * nz + e, half0, stride=2), :])
        rows += [blank] * (slots - len(rows))
        return jnp.concatenate(rows, axis=0).T

    for k in range(n0):
        both = lv0p.colours(pack(fn, k, 0), pack(fn, k, 1), k)
        ends = lv0p.colours(pack(fs, k, 0)[0 : 2 * SUB], pack(fs, k, 1)[0 : 2 * SUB], k)
        for c in (0, 1):
            f0q[c, k, HALO_Y : HALO_Y + ny, :] = both[c]
            f0q[c, k, 0:HALO_Y, :] = ends[c][0:SUB]
            f0q[c, k, HALO_Y + ny : tall0, :] = ends[c][SUB : 2 * SUB]

    tiles0 = tall0 // SUB
    lv0p.presmooth(p0, f0q, SWEEPS, tiles0, tiles0, False)
    lv0p.residual(p0, f0q, pairs, HALO_Y, ny // SUB, ny // SUB, False)

    own_x, nz1, half1 = nx // 2, nz // 2, nz // 4
    n1 = nx_dev * own_x * half1 // LANES
    lv1 = Packed(1, nz1, n1)
    wide = own_x // n1 * half1
    rows1 = ny // 2

    def down0(i, o):
        x = 2 * ((i % LANES) // half0 - side) + i // LANES
        z = i % half0
        place = ((z % 2) * n1 + x % n1) * wide + (x // n1) * half1 + z // 2
        return (x >= 0) & (x < own_x) & (place == o)

    sums = jnp.concatenate([pair_rows(pairs, j, rows1) for j in range(n0 // 2)], axis=1)
    gath[0, HALO_1 : HALO_1 + rows1, :] = mm(sums, matrix(LANES * (n0 // 2), LANES, 0.125, down0))
    body1 = slice(HALO_1, HALO_1 + rows1)
    copies = [send(gath.at[0, body1], gath.at[j, body1], nx_dev - j, 0) for j in range(1, nx_dev)]
    for j in range(nx_dev):
        copies.append(send(gath.at[0, rows1 : rows1 + HALO_1], gath.at[j, 0:HALO_1], nx_dev - j, 1))
        copies.append(
            send(gath.at[0, HALO_1 : 2 * HALO_1], gath.at[j, rows1 + HALO_1 : rows1 + 2 * HALO_1], nx_dev - j, -1)
        )

    own0 = SUB + HALO_Y
    for i in (0, 1):
        for r in range(0, ny, SUB):
            rows = slice(own0 + r, own0 + r + SUB)
            g, k = (side + blocks - 2, n0 - 1) if i == 0 else (side + 1, 0)
            out = pltpu.roll(p0[1, k, rows, :], ((n0 - g) * half0) % LANES, 1)
            g = side + blocks - 1 if i == 0 else side
            for m in range(n0):
                part = pltpu.roll(p0[1, m, rows, :], ((m - g) * half0) % LANES, 1)
                out = jnp.where(group == m, part, out)
            pk[i, r : r + SUB, :] = out
    for copy in copies:
        copy.wait()
    later = [
        send(p0.at[1, :, own0 + ny - SUB : own0 + ny, :], py_in.at[0], 0, 1),
        send(p0.at[1, :, own0 : own0 + SUB, :], py_in.at[1], 0, -1),
    ]
    for dx in (1, -1):
        i = 0 if dx > 0 else 1
        later.append(send(pk.at[i], pk_in.at[i, HALO_Y : HALO_Y + ny], dx, 0))
        later.append(send(pk.at[i, ny - SUB : ny], pk_in.at[i, 0:HALO_Y], dx, 1))
        later.append(send(pk.at[i, 0:SUB], pk_in.at[i, HALO_Y + ny : tall0], dx, -1))

    tall1 = rows1 + 2 * HALO_1
    source = iota2((SUB, LANES), 1) // wide

    def spread(r):
        parts = [gath[j, pl.ds(r, SUB), :] for j in range(nx_dev)]
        arr = []
        for m in range(2 * n1):
            out = pltpu.roll(parts[0], (-m * wide) % LANES, 1) if m else parts[0]
            for j in range(1, nx_dev):
                moved = pltpu.roll(parts[j], ((j - m) * wide) % LANES, 1) if j != m else parts[j]
                out = jnp.where(source == j, moved, out)
            arr.append(out)
        for k in range(n1):
            both = lv1.colours(arr[k], arr[n1 + k], k)
            f1[0, k, pl.ds(r, SUB), :] = both[0]
            f1[1, k, pl.ds(r, SUB), :] = both[1]

    tiles1 = tall1 // SUB
    row_loop(tiles1, tiles1, spread)
    lv1.presmooth(p1, f1, SWEEPS, tiles1, tiles1, False)
    lv1.residual(p1, f1, pairs, HALO_1, rows1 // SUB, rows1 // SUB, False)

    x2, nz2, half2 = nx_dev * nx // 4, nz // 4, nz // 8
    lanes2 = x2 * half2
    lv2 = Packed(2, nz2, 1)
    pieces = max(1, n1 // 2)
    own2 = ny // 4

    def down1(i, o):
        x = (i % LANES) // half1 * pieces + i // LANES
        z = i % half1
        return (z % 2) * lanes2 + x * half2 + z // 2 == o

    sums = jnp.concatenate([pair_rows(pairs, j, own2) for j in range(pieces)], axis=1)
    m2[0:own2, :] = mm(sums, matrix(LANES * pieces, 2 * lanes2, 0.125, down1))
    copies = [
        send(m2.at[0:own2, :], m2.at[j * own2 : (j + 1) * own2, :], 0, ny_dev - j) for j in range(1, ny_dev)
    ]
    for copy in copies:
        copy.wait()
    rows2 = ny_dev * own2
    low_half = iota2((SUB, LANES), 1) < LANES // 2

    def spread2(r):
        if lanes2 == LANES:
            even, odd = m2[pl.ds(r, SUB), 0:LANES], m2[pl.ds(r, SUB), LANES : 2 * LANES]
        else:
            both = m2[pl.ds(r, SUB), :]
            turned = pltpu.roll(both, LANES // 2, 1)
            even, odd = jnp.where(low_half, both, turned), jnp.where(low_half, turned, both)
        both = lv2.colours(even, odd, 0)
        f2[0, 0, pl.ds(r, SUB), :] = both[0]
        f2[1, 0, pl.ds(r, SUB), :] = both[1]

    row_loop(rows2 // SUB, 32, spread2)
    lv2.presmooth(p2, f2, SWEEPS, rows2 // SUB, 32, True)
    lv2.residual(p2, f2, pairs, 0, rows2 // SUB, 32, True)

    x3, half3 = x2 // 2, half2 // 2
    lv3 = Packed(3, nz2 // 2, 1)
    rows3 = rows2 // 2

    def down2(i, o):
        lane = o % LANES
        hit = (i < lanes2) & (i // half2 // 2 == (lane // half3) % x3)
        return hit & (i % half2 == 2 * (lane % half3) + o // LANES)

    down = mm(pair_rows(pairs, 0, rows3), matrix(LANES, 2 * LANES, 0.125, down2))
    both = lv3.colours(down[:, 0:LANES], down[:, LANES : 2 * LANES], 0)
    f3[0, 0] = both[0]
    f3[1, 0] = both[1]
    lv3.presmooth(p3, f3, COARSE_SWEEPS, rows3 // SUB, 16, True)

    def up3(i, o):
        lane = i % LANES
        hit = (lane < x3 * half3) & (lane // half3 == (o // half2) % x2 // 2)
        return hit & (2 * (lane % half3) + i // LANES == o % half2)

    inner3 = slice(SUB, SUB + rows3)
    both = lv3.colours(p3[0, 0, inner3, :], p3[1, 0, inner3, :], 0)
    twice_rows(mm(jnp.concatenate(both, axis=1), matrix(2 * LANES, LANES, 1.0, up3)), pairs, 0)
    p2[1, 0, SUB : SUB + rows2, :] += pairs[0, 0:rows2, :]
    lv2.postsmooth(p2, f2, 0, rows2 // SUB, 32, True)
    wrap_rows(p2, 0)
    wrap_rows(p2, 1)

    def up2(i, o):
        lane, to = i % LANES, o % LANES
        hit = (lane < lanes2) & (lane // half2 == (to // half1) * pieces + o // LANES)
        return hit & (2 * (lane % half2) + i // LANES == to % half1)

    first2 = SUB - HALO_1 // 2
    window = slice(first2, first2 + tall1 // 2)
    both = lv2.colours(p2[0, 0, window, :], p2[1, 0, window, :], 0)
    lift = mm(jnp.concatenate(both, axis=1), matrix(2 * LANES, LANES * pieces, 1.0, up2))
    for j in range(pieces):
        twice_rows(lift[:, tile_of(j)], pairs, j)
    for k in range(n1):
        p1[1, k, SUB : SUB + tall1, :] += pairs[k * pieces // n1, 0:tall1, :]
    lv1.postsmooth(p1, f1, 0, tiles1, tiles1, False)

    reach = side * n0 // 2
    wide_x = own_x + 2 * reach
    take = wide_x // n1 * half1
    off = -reach // n1 * half1
    first1 = SUB + HALO_1 - HALO_Y // 2
    window = slice(first1, first1 + tall0 // 2)
    halves = [[], []]
    for k in range(n1):
        both = lv1.colours(p1[0, k, window, :], p1[1, k, window, :], k)
        halves[0].append(both[0])
        halves[1].append(both[1])
    slot = iota2((tall0 // 2, LANES), 1) // take
    joined = []
    for e in (0, 1):
        out = None
        for k in range(n1):
            moved = pltpu.roll(halves[e][k], (k * take - off) % LANES, 1)
            out = moved if out is None else jnp.where(slot == k, moved, out)
        joined.append(out)

    def up1(i, o):
        lane, to = i % LANES, o % LANES
        x = (lane % take) // half1 * n1 + lane // take
        hit = (lane < take * n1) & (x == to // half0 * (n0 // 2) + o // LANES)
        return hit & (2 * (lane % half1) + i // LANES == to % half0)

    lift = mm(jnp.concatenate(joined, axis=1), matrix(2 * LANES, LANES * (n0 // 2), 1.0, up1))
    for j in range(n0 // 2):
        twice_rows(lift[:, tile_of(j)], pairs, j)
    for copy in later:
        copy.wait()
    for r in range(0, tall0, SUB):
        rows = slice(SUB + r, 2 * SUB + r)
        for k in range(n0):
            if r == 0 or r == HALO_Y + ny:
                value = py_in[0 if r == 0 else 1, k]
            else:
                value = p0[1, k, rows, :]
            for i in (0, 1):
                g = side - 1 if i == 0 else side + blocks
                part = pltpu.roll(pk_in[i, r : r + SUB, :], ((g - k) * half0) % LANES, 1)
                value = jnp.where(group == g, part, value)
                if k == (n0 - 1 if i == 0 else 0):
                    g = side - 2 if i == 0 else side + blocks + 1
                    part = pltpu.roll(pk_in[i, r : r + SUB, :], ((g - n0) * half0) % LANES, 1)
                    value = jnp.where(group == g, part, value)
            p0[1, k, rows, :] = value + pairs[k // 2, r : r + SUB, :]
    lv0p.postsmooth(p0, f0q, 0, tiles0, tiles0, False)

    low = SUB + HALO_Y
    body0 = slice(low, low + ny)
    ext = nx + 2 * HALO_X
    for k in range(n0):
        value = lv0p.colours(p0[0, k, body0, :], p0[1, k, body0, :], k)
        slope = [
            p0[1 - c, k, low + 1 : low + 1 + ny, :] - p0[1 - c, k, low - 1 : low - 1 + ny, :] for c in (0, 1)
        ]
        slope = lv0p.colours(slope[0], slope[1], k)
        for e in (0, 1):
            turned, sloped = value[e].T, slope[e].T
            for b in range(side - 1, side + blocks + 1):
                part = slice(b * half0, (b + 1) * half0)
                pn[pl.ds(e * ext + b * n0 + k, half0, stride=2 * ext), :] = turned[part, :]
                if side <= b < side + blocks:
                    gn[pl.ds(e * nx + (b - side) * n0 + k, half0, stride=2 * nx), :] = sloped[part, :]

    def correct(z):
        for h in range(nx // SUB):
            def cells(dz, dx):
                return pn[pl.ds((z + dz) * ext + HALO_X + h * SUB + dx, SUB), :]

            here = pl.ds(z * nx + h * SUB, SUB)
            pre_out[here, :] = cells(0, 0)
            wet = (1 - obs_in[here, :]).astype(jnp.float32)
            above = cells(1, 0) if z < nz - 1 else 0.0
            below = cells(-1, 0) if z > 0 else 0.0
            slope = (cells(0, 1) - cells(0, -1), gn[here, :], above - below)
            for c in range(3):
                there = pl.ds(c * nz * nx + z * nx + h * SUB, SUB)
                cor_out[there, :] = wet * (predn[there, :] - (0.5 * TIME_STEP) * slope[c])

    for z in range(nz):
        correct(z)


def body(nx_dev, ny_dev, velocity, old_tendency, obstacle):
    _, nz, nx, ny = velocity.shape
    width = nx * nz
    per = LANES // nz
    blocks = nx // per
    tall0 = ny + 2 * HALO_Y
    n1 = nx_dev * (nx // 2) * (nz // 4) // LANES
    tall1 = ny // 2 + 2 * HALO_1
    rows2 = ny_dev * ny // 4
    rows3 = rows2 // 2
    wide2 = 2 * (nx_dev * nx // 4) * (nz // 8)
    tall = max(tall0, tall1, rows2)
    count = max(per // 2, n1 // 2, 1)
    copies = 4 + 14 + 8 + (nx_dev - 1) + 2 * nx_dev + (ny_dev - 1)
    f32 = jnp.float32
    out = pl.pallas_call(
        functools.partial(kernel, nx_dev, ny_dev, nz, nx, ny),
        out_shape=(
            jax.ShapeDtypeStruct((3 * nz * nx, ny), f32),
            jax.ShapeDtypeStruct((nz * nx, ny), f32),
        ),
        in_specs=[pl.BlockSpec(memory_space=pltpu.VMEM)] * 3,
        out_specs=[pl.BlockSpec(memory_space=pltpu.VMEM)] * 2,
        scratch_shapes=[
            pltpu.VMEM((3, ny + 2 * SUB, width + 2 * LANES), f32),
            pltpu.VMEM((3, ny, width), f32),
            pltpu.VMEM((ny, width), f32),
            pltpu.VMEM((2, 3 * nz, ny), f32),
            pltpu.VMEM((2, 3 * nz, ny), f32),
            pltpu.VMEM((3, ny + 2 * SUB, width + 2 * LANES), f32),
            pltpu.VMEM((2, ny, LANES), f32),
            pltpu.VMEM((2, ny, LANES), f32),
            pltpu.VMEM((2, nz, ny), f32),
            pltpu.VMEM((2, nz, ny), f32),
            pltpu.VMEM((tall0, width + 2 * LANES), f32),
            pltpu.VMEM((blocks + 2, LANES, ny), f32),
            pltpu.VMEM((blocks + 2, LANES, ny), f32),
            pltpu.VMEM((2, per, tall0, LANES), f32),
            pltpu.VMEM((2, per, tall0 + 2 * SUB, LANES), f32),
            pltpu.VMEM((2, ny, LANES), f32),
            pltpu.VMEM((2, tall0, LANES), f32),
            pltpu.VMEM((2, per, SUB, LANES), f32),
            pltpu.VMEM((nx_dev, tall1, LANES), f32),
            pltpu.VMEM((2, n1, tall1, LANES), f32),
            pltpu.VMEM((2, n1, tall1 + 2 * SUB, LANES), f32),
            pltpu.VMEM((rows2, wide2), f32),
            pltpu.VMEM((2, 1, rows2, LANES), f32),
            pltpu.VMEM((2, 1, rows2 + 2 * SUB, LANES), f32),
            pltpu.VMEM((2, 1, rows3, LANES), f32),
            pltpu.VMEM((2, 1, rows3 + 2 * SUB, LANES), f32),
            pltpu.VMEM((count, tall, LANES), f32),
            pltpu.VMEM((3 * nz * nx, ny), f32),
            pltpu.VMEM((nz * (nx + 2 * HALO_X), ny), f32),
            pltpu.VMEM((nz * nx, ny), f32),
            pltpu.SemaphoreType.DMA((copies,)),
            pltpu.SemaphoreType.DMA((copies,)),
        ],
        compiler_params=pltpu.CompilerParams(
            collective_id=0, has_side_effects=True, vmem_limit_bytes=60 * 1024 * 1024
        ),
    )(
        velocity.reshape(3 * nz * nx, ny),
        old_tendency.reshape(3 * nz * nx, ny),
        obstacle.reshape(nz * nx, ny),
    )
    return out[0].reshape(3, nz, nx, ny), out[1].reshape(nz, nx, ny)


def solution(mesh):
    placed = (P(None, None, "gx", "gy"), P(None, None, "gx", "gy"), P(None, "gx", "gy"))
    return jax.shard_map(
        functools.partial(body, mesh.shape["gx"], mesh.shape["gy"]),
        mesh=mesh,
        in_specs=placed,
        out_specs=(P(None, None, "gx", "gy"), P(None, "gx", "gy")),
        check_vma=False,
    )
```

```python
import functools

import jax
import jax.numpy as jnp
from jax import lax
from jax.experimental import pallas as pl
from jax.experimental.pallas import tpu as pltpu
from jax.sharding import PartitionSpec as P

LEVELS = 3
SWEEPS = 2
COARSE_SWEEPS = 8
VISCOSITY = 0.1
TIME_STEP = 0.25
WEIGHT_NEW = 15.0 / 16.0
WEIGHT_OLD = -25.0 / 48.0
HELMHOLTZ = 0.0001

LANES = 128
SUB = 8
HALO_X = 8
HALO_Y = 8
HALO_1 = 8
MESH = pl.DeviceIdType.MESH


def iota2(shape, dim):
    return lax.broadcasted_iota(jnp.int32, shape, dim)


def mm(a, b):
    return jnp.dot(a, b, precision=lax.Precision.HIGHEST, preferred_element_type=jnp.float32)


class Level:
    def __init__(self, level, nz):
        self.nz = nz
        self.scale = 1.0 / float(4**level)
        lane = iota2((SUB, LANES), 1)
        row = iota2((SUB, LANES), 0)
        self.lane = lane
        self.row = row
        z = lane % nz
        self.not_top = z < nz - 1
        self.not_bottom = z > 0
        parity = (z + lane // nz + row) % 2
        self.colour = [parity == 0, parity == 1]
        edge = (z == 0) | (z == nz - 1)
        diag_in = HELMHOLTZ + 6.0 * self.scale
        diag_edge = HELMHOLTZ + 5.0 * self.scale
        self.diag = jnp.where(edge, diag_edge, diag_in).astype(jnp.float32)
        self.inv = jnp.where(edge, 1.0 / diag_edge, 1.0 / diag_in).astype(jnp.float32)
        self.take = jnp.where(
            edge, self.scale / diag_edge, self.scale / diag_in
        ).astype(jnp.float32)

    def x_plus(self, tiles, t):
        n = len(tiles)
        both = tiles[t] if n == 1 else jnp.where(self.lane < self.nz, tiles[(t + 1) % n], tiles[t])
        return pltpu.roll(both, LANES - self.nz, 1)

    def x_minus(self, tiles, t):
        n = len(tiles)
        last = self.lane >= LANES - self.nz
        both = tiles[t] if n == 1 else jnp.where(last, tiles[(t - 1) % n], tiles[t])
        return pltpu.roll(both, self.nz, 1)

    def y_plus(self, tile, following):
        return pltpu.roll(jnp.where(self.row == 0, following, tile), SUB - 1, 0)

    def y_minus(self, tile, previous):
        return pltpu.roll(jnp.where(self.row == SUB - 1, previous, tile), 1, 0)

    def z_plus(self, tile):
        return jnp.where(self.not_top, pltpu.roll(tile, LANES - 1, 1), 0.0)

    def z_minus(self, tile):
        return jnp.where(self.not_bottom, pltpu.roll(tile, 1, 1), 0.0)


def tile_of(t):
    return slice(t * LANES, (t + 1) * LANES)


def row_loop(tiles, unroll, body):
    while tiles % unroll:
        unroll -= 1

    def step(i, carry):
        for k in range(unroll):
            body(pl.multiple_of((i * unroll + k) * SUB, SUB))
        return carry

    lax.fori_loop(0, tiles // unroll, step, 0)


class Packed:
    def __init__(self, level, nz, n):
        self.n = n
        self.half = half = nz // 2
        self.scale = scale = 1.0 / float(4**level)
        lane, row = iota2((SUB, LANES), 1), iota2((SUB, LANES), 0)
        zh = lane % half
        diag_in, diag_edge = HELMHOLTZ + 6.0 * scale, HELMHOLTZ + 5.0 * scale
        odd = ((lane // half) * n + row) % 2 == 1
        self.odd = [odd, ~odd]
        self.up, self.down, self.diag, self.inv, self.take = [], [], [], [], []
        for v in (0, 1):
            up = self.odd[v] & (zh < half - 1)
            down = self.odd[1 - v] & (zh > 0)
            inside = up | down
            self.up.append(up)
            self.down.append(down)
            self.diag.append(jnp.where(inside, diag_in, diag_edge).astype(jnp.float32))
            self.inv.append(jnp.where(inside, 1.0 / diag_in, 1.0 / diag_edge).astype(jnp.float32))
            self.take.append(jnp.where(inside, scale / diag_in, scale / diag_edge).astype(jnp.float32))

    def totals(self, q, other, r):
        n = self.n
        here = [q[other, k, pl.ds(r, SUB), :] for k in range(n)]
        first = pltpu.roll(here[0], LANES - self.half, 1)
        last = pltpu.roll(here[n - 1], self.half, 1)
        out = []
        for k in range(n):
            v = (k + 1 - other) % 2
            b = here[k]
            east = here[k + 1] if k < n - 1 else first
            west = here[k - 1] if k > 0 else last
            north = q[other, k, pl.ds(r + 1, SUB), :]
            south = q[other, k, pl.ds(r - 1, SUB), :]
            z = jnp.where(
                self.up[v],
                pltpu.roll(b, LANES - 1, 1),
                jnp.where(self.down[v], pltpu.roll(b, 1, 1), 0.0),
            )
            out.append((east + west) + (north + south) + (b + z))
        return out

    def first(self, q, f, start, count, unroll):
        def body(i):
            for k in range(self.n):
                r = i + start
                q[0, k, pl.ds(r + SUB, SUB), :] = f[0, k, pl.ds(r, SUB), :] * self.inv[k % 2]

        row_loop(count, unroll, body)

    def half_sweep(self, q, f, c, start, count, unroll, wrap):
        if wrap:
            wrap_rows(q, 1 - c)

        def body(i):
            r = i + start
            total = self.totals(q, 1 - c, r + SUB)
            for k in range(self.n):
                v = (k + c) % 2
                q[c, k, pl.ds(r + SUB, SUB), :] = (
                    f[c, k, pl.ds(r, SUB), :] * self.inv[v] + total[k] * self.take[v]
                )

        row_loop(count, unroll, body)

    def presmooth(self, q, f, sweeps, count, unroll, wrap):
        self.first(q, f, 0, count, unroll)
        for k in range(1, 2 * sweeps):
            self.half_sweep(q, f, k % 2, 0, count, unroll, wrap)

    def postsmooth(self, q, f, start, count, unroll, wrap):
        for k in range(2 * SWEEPS):
            self.half_sweep(q, f, k % 2, start, count, unroll, wrap)

    def residual(self, q, f, out, start, count, unroll, wrap):
        if wrap:
            wrap_rows(q, 0)
            wrap_rows(q, 1)
        n = self.n

        def body(i):
            r = i + start
            parts = [None] * n
            for c in (0, 1):
                total = self.totals(q, 1 - c, r + SUB)
                for k in range(n):
                    v = (k + c) % 2
                    res = f[c, k, pl.ds(r, SUB), :] - (
                        self.diag[v] * q[c, k, pl.ds(r + SUB, SUB), :] - self.scale * total[k]
                    )
                    parts[k] = res if c == 0 else parts[k] + res
            if n == 1:
                out[0, pl.ds(i, SUB), :] = parts[0]
            else:
                for j in range(n // 2):
                    out[j, pl.ds(i, SUB), :] = parts[2 * j] + parts[2 * j + 1]

        row_loop(count, unroll, body)

    def colours(self, even, odd, k):
        rows = even.shape[0]
        odd_cell = jnp.concatenate([self.odd[k % 2]] * (rows // SUB), axis=0)
        return jnp.where(odd_cell, odd, even), jnp.where(odd_cell, even, odd)


def wrap_rows(q, c):
    rows = q.shape[2]
    for k in range(q.shape[1]):
        q[c, k, 0:SUB, :] = q[c, k, rows - 2 * SUB : rows - SUB, :]
        q[c, k, rows - SUB : rows, :] = q[c, k, SUB : 2 * SUB, :]


def pair_rows(ref, j, rows):
    return ref[j, pl.ds(0, rows, stride=2), :] + ref[j, pl.ds(1, rows, stride=2), :]


def twice_rows(value, pairs, j):
    rows = value.shape[0]
    pairs[j, pl.ds(0, rows, stride=2), :] = value
    pairs[j, pl.ds(1, rows, stride=2), :] = value


def matrix(rows, cols, weight, hit):
    i, o = iota2((rows, cols), 0), iota2((rows, cols), 1)
    return jnp.where(hit(i, o), weight, 0.0).astype(jnp.float32)


def kernel(
    nx_dev, ny_dev, nz, nx, ny,
    vel_in, old_in, obs_in, predn, pn, gn,
    vel, old, fluid, edge, edge_in, pred,
    fe, fe_in, pe, pe_in, f0, fn, fs, f0q, p0, pk, pk_in, py_in, p1y_in,
    gath, f1, p1, m2, f2, p2, f3, p3, pairs, send_sem, recv_sem,
):
    gx, gy = lax.axis_index("gx"), lax.axis_index("gy")

    def device(dx, dy):
        return (lax.rem(gx + dx + nx_dev, nx_dev), lax.rem(gy + dy + ny_dev, ny_dev))

    peers = [(d, 0) for d in range(1, nx_dev)] + [(0, d) for d in range(1, ny_dev)]
    peers += [(a, b) for a in range(1, nx_dev) for b in (-1, 1)]
    barrier = pltpu.get_barrier_semaphore()
    for dx, dy in peers:
        pl.semaphore_signal(barrier, inc=1, device_id=device(dx, dy), device_id_type=MESH)

    number = [0]

    def send(src, dst, dx, dy):
        k = number[0]
        number[0] += 1
        copy = pltpu.make_async_remote_copy(
            src_ref=src, dst_ref=dst, send_sem=send_sem.at[k], recv_sem=recv_sem.at[k],
            device_id=device(dx, dy), device_id_type=MESH,
        )
        copy.start()
        return copy

    per = LANES // nz
    blocks = nx // per
    width = blocks * LANES
    lv0 = Level(0, nz)
    lane = lv0.lane

    def load_tile(ref, base, t):
        rows = [ref[pl.ds(base + t * per + i, nz, stride=nx), :] for i in range(per)]
        return jnp.concatenate(rows, axis=0).T

    for i in (0, 1):
        for c in range(3):
            edge[i, c * nz : (c + 1) * nz, :] = vel_in[
                pl.ds(c * nz * nx + (nx - 1 if i == 0 else 0), nz, stride=nx), :
            ]
    for c in range(3):
        for t in range(blocks):
            vel[c, SUB : SUB + ny, tile_of(t + 1)] = load_tile(vel_in, c * nz * nx, t)

    pltpu_wait = functools.partial(pl.semaphore_wait, barrier)
    pltpu_wait(len(peers))

    copies = [
        send(edge.at[0], edge_in.at[0], 1, 0),
        send(edge.at[1], edge_in.at[1], -1, 0),
        send(vel.at[:, ny : ny + SUB, LANES : LANES + width], vel.at[:, 0:SUB, LANES : LANES + width], 0, 1),
        send(
            vel.at[:, SUB : 2 * SUB, LANES : LANES + width],
            vel.at[:, SUB + ny : 2 * SUB + ny, LANES : LANES + width], 0, -1,
        ),
    ]

    for c in range(3):
        for t in range(blocks):
            old[c, :, tile_of(t)] = load_tile(old_in, c * nz * nx, t)
    for t in range(blocks):
        fluid[:, tile_of(t)] = (1 - load_tile(obs_in, 0, t)).astype(jnp.float32)
    for copy in copies:
        copy.wait()
    rest = jnp.zeros((LANES - 3 * nz, ny), jnp.float32)
    beside = [jnp.concatenate([edge_in[i], rest], axis=0).T for i in (0, 1)]
    for c in range(3):
        vel[c, SUB : SUB + ny, tile_of(0)] = pltpu.roll(beside[0], (LANES - nz - c * nz) % LANES, 1)
        vel[c, SUB : SUB + ny, tile_of(blocks + 1)] = pltpu.roll(beside[1], (-c * nz) % LANES, 1)

    def momentum(r):
        here = [
            [vel[c, pl.ds(r + SUB, SUB), tile_of(t)] for t in range(blocks + 2)] for c in range(3)
        ]
        for t in range(1, blocks + 1):
            cols = tile_of(t)
            wet = fluid[pl.ds(r, SUB), tile_of(t - 1)]
            for c in range(3):
                q = here[c][t]
                xp, xm = lv0.x_plus(here[c], t), lv0.x_minus(here[c], t)
                yp = lv0.y_plus(q, vel[c, pl.ds(r + 2 * SUB, SUB), cols])
                ym = lv0.y_minus(q, vel[c, pl.ds(r, SUB), cols])
                zp, zm = lv0.z_plus(q), lv0.z_minus(q)
                advect = 0.5 * (
                    here[0][t] * (xp - xm) + here[1][t] * (yp - ym) + here[2][t] * (zp - zm)
                )
                diffuse = xp + xm + yp + ym + zp + zm - 6.0 * q
                tendency = VISCOSITY * diffuse - advect
                pred[c, pl.ds(r + SUB, SUB), cols] = wet * (
                    q
                    + TIME_STEP
                    * (WEIGHT_NEW * tendency + WEIGHT_OLD * old[c, pl.ds(r, SUB), tile_of(t - 1)])
                )

    row_loop(ny // SUB, 16, momentum)

    inner = slice(LANES, LANES + width)
    own_rows = slice(SUB, SUB + ny)
    factor = 0.5 / TIME_STEP
    side = HALO_X // per
    none = jnp.zeros((SUB, LANES), jnp.float32)

    def source_of(r, t, whole):
        cols = tile_of(t)
        rows = pl.ds(r, SUB)
        first, last = r == (0 if whole else SUB), r == (SUB + ny if whole else ny)
        u = [pred[0, rows, tile_of(i)] for i in range(blocks + 2)] if whole else (
            [none] + [pred[0, rows, tile_of(i)] for i in range(1, blocks + 1)] + [none]
        )
        v, w = pred[1, rows, cols], pred[2, rows, cols]
        north = none if last else pred[1, pl.ds(r + SUB, SUB), cols]
        south = none if first else pred[1, pl.ds(r - SUB, SUB), cols]
        total = (
            (lv0.x_plus(u, t) - lv0.x_minus(u, t))
            + (lv0.y_plus(v, north) - lv0.y_minus(v, south))
            + (lv0.z_plus(w) - lv0.z_minus(w))
        )
        return total * (-factor)

    def turn_rows(ref, base, t, turned):
        for i in range(per):
            ref[pl.ds(base + t * per + i, nz, stride=nx), :] = turned[i * nz : (i + 1) * nz, :]

    copies = [
        send(pred.at[:, ny : ny + SUB, inner], pred.at[:, 0:SUB, inner], 0, 1),
        send(pred.at[:, SUB : 2 * SUB, inner], pred.at[:, SUB + ny : 2 * SUB + ny, inner], 0, -1),
    ]
    for dx in (1, -1):
        i, t = (0, blocks) if dx > 0 else (1, 1)
        for r in range(0, ny, SUB):
            fe[i, r : r + SUB, :] = source_of(r + SUB, t, False)
        copies.append(send(fe.at[i], fe_in.at[i], dx, 0))
        turned = pred[0, own_rows, tile_of(t)].T
        pe[i] = turned[LANES - nz : LANES, :] if dx > 0 else turned[0:nz, :]
        copies.append(send(pe.at[i], pe_in.at[i], dx, 0))
        for dy in (1, -1):
            rows = slice(ny, ny + SUB) if dy > 0 else slice(SUB, 2 * SUB)
            there = slice(0, SUB) if dy > 0 else slice(SUB + ny, 2 * SUB + ny)
            copies.append(
                send(pred.at[:, rows, tile_of(t)], pred.at[:, there, tile_of(0 if dx > 0 else blocks + 1)], dx, dy)
            )
            copies.append(
                send(pred.at[1, rows, tile_of(t)], pred.at[1, rows, tile_of(0 if dx > 0 else blocks + 1)], dx, 0)
            )

    n0, half0 = per, nz // 2
    lv0p = Packed(0, nz, n0)
    tall0 = ny + 2 * HALO_Y
    blank = jnp.zeros((half0, ny), jnp.float32)
    group = iota2((SUB, LANES), 1) // half0
    slots = LANES // half0
    corners = [(a, b) for a in (1, -1) for b in (1, -1)]

    for c in range(3):
        for t in range(blocks):
            turn_rows(predn, c * nz * nx, t, pred[c, own_rows, tile_of(t + 1)].T)

    p0[...] = jnp.zeros(p0.shape, jnp.float32)
    p1[...] = jnp.zeros(p1.shape, jnp.float32)
    for copy in copies:
        copy.wait()

    blanks = jnp.zeros((LANES - nz, ny), jnp.float32)
    pred[0, own_rows, tile_of(0)] = jnp.concatenate([blanks, pe_in[0]], axis=0).T
    pred[0, own_rows, tile_of(blocks + 1)] = jnp.concatenate([pe_in[1], blanks], axis=0).T
    for r in range(0, tall0, SUB):
        strip = r == 0 or r == SUB + ny
        for t in range(blocks + 2):
            if strip or 1 <= t <= blocks:
                f0[r : r + SUB, tile_of(t)] = source_of(r, t, True)
                continue
            i = 0 if t == 0 else 1
            value = fe_in[i, r - SUB : r, :]
            near = pltpu.roll(
                pred[0, r : r + SUB, tile_of(1 if i == 0 else blocks)], LANES - nz if i == 0 else nz, 1
            )
            if i == 0:
                value = value - jnp.where(lane >= LANES - nz, factor * near, 0.0)
            else:
                value = value + jnp.where(lane < nz, factor * near, 0.0)
            if r == SUB:
                south = pltpu.roll(pred[1, 0:SUB, tile_of(t)], 1, 0)
                value = value + jnp.where(lv0.row == 0, factor * south, 0.0)
            if r == ny:
                north = pltpu.roll(pred[1, SUB + ny : 2 * SUB + ny, tile_of(t)], SUB - 1, 0)
                value = value - jnp.where(lv0.row == SUB - 1, factor * north, 0.0)
            f0[r : r + SUB, tile_of(t)] = value

    for t in range(blocks + 2):
        fn[t] = f0[own_rows, tile_of(t)].T
        strips = [f0[0:SUB, tile_of(t)], f0[SUB + ny : 2 * SUB + ny, tile_of(t)]]
        fs[t] = jnp.concatenate(strips + [jnp.zeros((LANES - 2 * SUB, LANES), jnp.float32)], axis=0).T

    def pack(ref, k, e):
        rows = [blank] * (side - 1)
        for t in range(blocks + 2):
            rows.append(ref[t, pl.ds(k * nz + e, half0, stride=2), :])
        rows += [blank] * (slots - len(rows))
        return jnp.concatenate(rows, axis=0).T

    for k in range(n0):
        both = lv0p.colours(pack(fn, k, 0), pack(fn, k, 1), k)
        ends = lv0p.colours(pack(fs, k, 0)[0 : 2 * SUB], pack(fs, k, 1)[0 : 2 * SUB], k)
        for c in (0, 1):
            f0q[c, k, HALO_Y : HALO_Y + ny, :] = both[c]
            f0q[c, k, 0:HALO_Y, :] = ends[c][0:SUB]
            f0q[c, k, HALO_Y + ny : tall0, :] = ends[c][SUB : 2 * SUB]

    tiles0 = tall0 // SUB
    lv0p.presmooth(p0, f0q, SWEEPS, tiles0, tiles0, False)
    lv0p.residual(p0, f0q, pairs, HALO_Y, ny // SUB, ny // SUB, False)

    own_x, nz1, half1 = nx // 2, nz // 2, nz // 4
    n1 = nx_dev * own_x * half1 // LANES
    lv1 = Packed(1, nz1, n1)
    wide = own_x // n1 * half1
    rows1 = ny // 2

    def down0(i, o):
        x = 2 * ((i % LANES) // half0 - side) + i // LANES
        z = i % half0
        place = ((z % 2) * n1 + x % n1) * wide + (x // n1) * half1 + z // 2
        return (x >= 0) & (x < own_x) & (place == o)

    sums = jnp.concatenate([pair_rows(pairs, j, rows1) for j in range(n0 // 2)], axis=1)
    gath[0, HALO_1 : HALO_1 + rows1, :] = mm(sums, matrix(LANES * (n0 // 2), LANES, 0.125, down0))
    body1 = slice(HALO_1, HALO_1 + rows1)
    copies = [send(gath.at[0, body1], gath.at[j, body1], nx_dev - j, 0) for j in range(1, nx_dev)]
    for j in range(nx_dev):
        copies.append(send(gath.at[0, rows1 : rows1 + HALO_1], gath.at[j, 0:HALO_1], nx_dev - j, 1))
        copies.append(
            send(gath.at[0, HALO_1 : 2 * HALO_1], gath.at[j, rows1 + HALO_1 : rows1 + 2 * HALO_1], nx_dev - j, -1)
        )

    own0 = SUB + HALO_Y
    for i in (0, 1):
        for r in range(0, ny, SUB):
            rows = slice(own0 + r, own0 + r + SUB)
            g, k = (side + blocks - 2, n0 - 1) if i == 0 else (side + 1, 0)
            out = pltpu.roll(p0[1, k, rows, :], ((n0 - g) * half0) % LANES, 1)
            g = side + blocks - 1 if i == 0 else side
            for m in range(n0):
                part = pltpu.roll(p0[1, m, rows, :], ((m - g) * half0) % LANES, 1)
                out = jnp.where(group == m, part, out)
            pk[i, r : r + SUB, :] = out
    for copy in copies:
        copy.wait()
    later = [
        send(p0.at[1, :, own0 + ny - SUB : own0 + ny, :], py_in.at[0], 0, 1),
        send(p0.at[1, :, own0 : own0 + SUB, :], py_in.at[1], 0, -1),
    ]
    for dx in (1, -1):
        i = 0 if dx > 0 else 1
        later.append(send(pk.at[i], pk_in.at[i, HALO_Y : HALO_Y + ny], dx, 0))
        later.append(send(pk.at[i, ny - SUB : ny], pk_in.at[i, 0:HALO_Y], dx, 1))
        later.append(send(pk.at[i, 0:SUB], pk_in.at[i, HALO_Y + ny : tall0], dx, -1))

    tall1 = rows1 + 2 * HALO_1
    source = iota2((SUB, LANES), 1) // wide

    def spread(r):
        parts = [gath[j, pl.ds(r, SUB), :] for j in range(nx_dev)]
        arr = []
        for m in range(2 * n1):
            out = pltpu.roll(parts[0], (-m * wide) % LANES, 1) if m else parts[0]
            for j in range(1, nx_dev):
                moved = pltpu.roll(parts[j], ((j - m) * wide) % LANES, 1) if j != m else parts[j]
                out = jnp.where(source == j, moved, out)
            arr.append(out)
        for k in range(n1):
            both = lv1.colours(arr[k], arr[n1 + k], k)
            f1[0, k, pl.ds(r, SUB), :] = both[0]
            f1[1, k, pl.ds(r, SUB), :] = both[1]

    tiles1 = tall1 // SUB
    row_loop(tiles1, tiles1, spread)
    lv1.presmooth(p1, f1, SWEEPS, tiles1, tiles1, False)
    lv1.residual(p1, f1, pairs, HALO_1, rows1 // SUB, rows1 // SUB, False)

    x2, nz2, half2 = nx_dev * nx // 4, nz // 4, nz // 8
    lanes2 = x2 * half2
    lv2 = Packed(2, nz2, 1)
    pieces = max(1, n1 // 2)
    own2 = ny // 4

    def down1(i, o):
        x = (i % LANES) // half1 * pieces + i // LANES
        z = i % half1
        return (z % 2) * lanes2 + x * half2 + z // 2 == o

    sums = jnp.concatenate([pair_rows(pairs, j, own2) for j in range(pieces)], axis=1)
    m2[0:own2, :] = mm(sums, matrix(LANES * pieces, 2 * lanes2, 0.125, down1))
    copies = [
        send(m2.at[0:own2, :], m2.at[j * own2 : (j + 1) * own2, :], 0, ny_dev - j) for j in range(1, ny_dev)
    ]
    own1 = SUB + HALO_1
    beyond = [
        send(p1.at[1, :, own1 + rows1 - HALO_1 : own1 + rows1, :], p1y_in.at[0], 0, 1),
        send(p1.at[1, :, own1 : own1 + HALO_1, :], p1y_in.at[1], 0, -1),
    ]
    for copy in copies:
        copy.wait()
    rows2 = ny_dev * own2
    low_half = iota2((SUB, LANES), 1) < LANES // 2

    def spread2(r):
        if lanes2 == LANES:
            even, odd = m2[pl.ds(r, SUB), 0:LANES], m2[pl.ds(r, SUB), LANES : 2 * LANES]
        else:
            both = m2[pl.ds(r, SUB), :]
            turned = pltpu.roll(both, LANES // 2, 1)
            even, odd = jnp.where(low_half, both, turned), jnp.where(low_half, turned, both)
        both = lv2.colours(even, odd, 0)
        f2[0, 0, pl.ds(r, SUB), :] = both[0]
        f2[1, 0, pl.ds(r, SUB), :] = both[1]

    row_loop(rows2 // SUB, 32, spread2)
    lv2.presmooth(p2, f2, SWEEPS, rows2 // SUB, 32, True)
    lv2.residual(p2, f2, pairs, 0, rows2 // SUB, 32, True)

    x3, half3 = x2 // 2, half2 // 2
    lv3 = Packed(3, nz2 // 2, 1)
    rows3 = rows2 // 2

    def down2(i, o):
        lane = o % LANES
        hit = (i < lanes2) & (i // half2 // 2 == (lane // half3) % x3)
        return hit & (i % half2 == 2 * (lane % half3) + o // LANES)

    down = mm(pair_rows(pairs, 0, rows3), matrix(LANES, 2 * LANES, 0.125, down2))
    both = lv3.colours(down[:, 0:LANES], down[:, LANES : 2 * LANES], 0)
    f3[0, 0] = both[0]
    f3[1, 0] = both[1]
    lv3.presmooth(p3, f3, COARSE_SWEEPS, rows3 // SUB, 16, True)

    def up3(i, o):
        lane = i % LANES
        hit = (lane < x3 * half3) & (lane // half3 == (o // half2) % x2 // 2)
        return hit & (2 * (lane % half3) + i // LANES == o % half2)

    inner3 = slice(SUB, SUB + rows3)
    both = lv3.colours(p3[0, 0, inner3, :], p3[1, 0, inner3, :], 0)
    twice_rows(mm(jnp.concatenate(both, axis=1), matrix(2 * LANES, LANES, 1.0, up3)), pairs, 0)
    p2[1, 0, SUB : SUB + rows2, :] += pairs[0, 0:rows2, :]
    lv2.postsmooth(p2, f2, 0, rows2 // SUB, 32, True)
    wrap_rows(p2, 0)
    wrap_rows(p2, 1)

    def up2(i, o):
        lane, to = i % LANES, o % LANES
        hit = (lane < lanes2) & (lane // half2 == (to // half1) * pieces + o // LANES)
        return hit & (2 * (lane % half2) + i // LANES == to % half1)

    first2 = SUB - HALO_1 // 2
    window = slice(first2, first2 + tall1 // 2)
    both = lv2.colours(p2[0, 0, window, :], p2[1, 0, window, :], 0)
    lift = mm(jnp.concatenate(both, axis=1), matrix(2 * LANES, LANES * pieces, 1.0, up2))
    for j in range(pieces):
        twice_rows(lift[:, tile_of(j)], pairs, j)
    for copy in beyond:
        copy.wait()
    for k in range(n1):
        p1[1, k, SUB : SUB + HALO_1, :] = p1y_in[0, k]
        p1[1, k, own1 + rows1 : own1 + rows1 + HALO_1, :] = p1y_in[1, k]
        p1[1, k, SUB : SUB + tall1, :] += pairs[k * pieces // n1, 0:tall1, :]
    lv1.postsmooth(p1, f1, 0, tiles1, tiles1, False)

    reach = side * n0 // 2
    wide_x = own_x + 2 * reach
    take = wide_x // n1 * half1
    off = -reach // n1 * half1
    first1 = SUB + HALO_1 - HALO_Y // 2
    window = slice(first1, first1 + tall0 // 2)
    halves = [[], []]
    for k in range(n1):
        both = lv1.colours(p1[0, k, window, :], p1[1, k, window, :], k)
        halves[0].append(both[0])
        halves[1].append(both[1])
    slot = iota2((tall0 // 2, LANES), 1) // take
    joined = []
    for e in (0, 1):
        out = None
        for k in range(n1):
            moved = pltpu.roll(halves[e][k], (k * take - off) % LANES, 1)
            out = moved if out is None else jnp.where(slot == k, moved, out)
        joined.append(out)

    def up1(i, o):
        lane, to = i % LANES, o % LANES
        x = (lane % take) // half1 * n1 + lane // take
        hit = (lane < take * n1) & (x == to // half0 * (n0 // 2) + o // LANES)
        return hit & (2 * (lane % half1) + i // LANES == to % half0)

    lift = mm(jnp.concatenate(joined, axis=1), matrix(2 * LANES, LANES * (n0 // 2), 1.0, up1))
    for j in range(n0 // 2):
        twice_rows(lift[:, tile_of(j)], pairs, j)
    for copy in later:
        copy.wait()
    for r in range(0, tall0, SUB):
        rows = slice(SUB + r, 2 * SUB + r)
        for k in range(n0):
            if r == 0 or r == HALO_Y + ny:
                value = py_in[0 if r == 0 else 1, k]
            else:
                value = p0[1, k, rows, :]
            for i in (0, 1):
                g = side - 1 if i == 0 else side + blocks
                part = pltpu.roll(pk_in[i, r : r + SUB, :], ((g - k) * half0) % LANES, 1)
                value = jnp.where(group == g, part, value)
                if k == (n0 - 1 if i == 0 else 0):
                    g = side - 2 if i == 0 else side + blocks + 1
                    part = pltpu.roll(pk_in[i, r : r + SUB, :], ((g - n0) * half0) % LANES, 1)
                    value = jnp.where(group == g, part, value)
            p0[1, k, rows, :] = value + pairs[k // 2, r : r + SUB, :]
    lv0p.postsmooth(p0, f0q, 0, tiles0, tiles0, False)

    low = SUB + HALO_Y
    body0 = slice(low, low + ny)
    ext = nx + 2 * HALO_X
    for k in range(n0):
        value = lv0p.colours(p0[0, k, body0, :], p0[1, k, body0, :], k)
        slope = [
            p0[1 - c, k, low + 1 : low + 1 + ny, :] - p0[1 - c, k, low - 1 : low - 1 + ny, :] for c in (0, 1)
        ]
        slope = lv0p.colours(slope[0], slope[1], k)
        for e in (0, 1):
            turned, sloped = value[e].T, slope[e].T
            for b in range(side - 1, side + blocks + 1):
                part = slice(b * half0, (b + 1) * half0)
                pn[pl.ds(e * ext + b * n0 + k, half0, stride=2 * ext), :] = turned[part, :]
                if side <= b < side + blocks:
                    gn[pl.ds(e * nx + (b - side) * n0 + k, half0, stride=2 * nx), :] = sloped[part, :]


def finish(nz, nx, predn, pn, gn, obs_in, cor_out, pre_out):
    ext = nx + 2 * HALO_X

    def correct(z):
        for h in range(nx // SUB):
            def cells(dz, dx):
                return pn[pl.ds((z + dz) * ext + HALO_X + h * SUB + dx, SUB), :]

            here = pl.ds(z * nx + h * SUB, SUB)
            pre_out[here, :] = cells(0, 0)
            wet = (1 - obs_in[here, :]).astype(jnp.float32)
            above = cells(1, 0) if z < nz - 1 else 0.0
            below = cells(-1, 0) if z > 0 else 0.0
            slope = (cells(0, 1) - cells(0, -1), gn[here, :], above - below)
            for c in range(3):
                there = pl.ds(c * nz * nx + z * nx + h * SUB, SUB)
                cor_out[there, :] = wet * (predn[there, :] - (0.5 * TIME_STEP) * slope[c])

    for z in range(nz):
        correct(z)


def body(nx_dev, ny_dev, velocity, old_tendency, obstacle):
    _, nz, nx, ny = velocity.shape
    width = nx * nz
    per = LANES // nz
    blocks = nx // per
    tall0 = ny + 2 * HALO_Y
    n1 = nx_dev * (nx // 2) * (nz // 4) // LANES
    tall1 = ny // 2 + 2 * HALO_1
    rows2 = ny_dev * ny // 4
    rows3 = rows2 // 2
    wide2 = 2 * (nx_dev * nx // 4) * (nz // 8)
    tall = max(tall0, tall1, rows2)
    count = max(per // 2, n1 // 2, 1)
    copies = 4 + 14 + 8 + (nx_dev - 1) + 2 * nx_dev + (ny_dev - 1) + 2
    f32 = jnp.float32
    parts = pl.pallas_call(
        functools.partial(kernel, nx_dev, ny_dev, nz, nx, ny),
        out_shape=(
            jax.ShapeDtypeStruct((3 * nz * nx, ny), f32),
            jax.ShapeDtypeStruct((nz * (nx + 2 * HALO_X), ny), f32),
            jax.ShapeDtypeStruct((nz * nx, ny), f32),
        ),
        in_specs=[pl.BlockSpec(memory_space=pltpu.VMEM)] * 3,
        out_specs=[pl.BlockSpec(memory_space=pltpu.VMEM)] * 3,
        scratch_shapes=[
            pltpu.VMEM((3, ny + 2 * SUB, width + 2 * LANES), f32),
            pltpu.VMEM((3, ny, width), f32),
            pltpu.VMEM((ny, width), f32),
            pltpu.VMEM((2, 3 * nz, ny), f32),
            pltpu.VMEM((2, 3 * nz, ny), f32),
            pltpu.VMEM((3, ny + 2 * SUB, width + 2 * LANES), f32),
            pltpu.VMEM((2, ny, LANES), f32),
            pltpu.VMEM((2, ny, LANES), f32),
            pltpu.VMEM((2, nz, ny), f32),
            pltpu.VMEM((2, nz, ny), f32),
            pltpu.VMEM((tall0, width + 2 * LANES), f32),
            pltpu.VMEM((blocks + 2, LANES, ny), f32),
            pltpu.VMEM((blocks + 2, LANES, ny), f32),
            pltpu.VMEM((2, per, tall0, LANES), f32),
            pltpu.VMEM((2, per, tall0 + 2 * SUB, LANES), f32),
            pltpu.VMEM((2, ny, LANES), f32),
            pltpu.VMEM((2, tall0, LANES), f32),
            pltpu.VMEM((2, per, SUB, LANES), f32),
            pltpu.VMEM((2, n1, HALO_1, LANES), f32),
            pltpu.VMEM((nx_dev, tall1, LANES), f32),
            pltpu.VMEM((2, n1, tall1, LANES), f32),
            pltpu.VMEM((2, n1, tall1 + 2 * SUB, LANES), f32),
            pltpu.VMEM((rows2, wide2), f32),
            pltpu.VMEM((2, 1, rows2, LANES), f32),
            pltpu.VMEM((2, 1, rows2 + 2 * SUB, LANES), f32),
            pltpu.VMEM((2, 1, rows3, LANES), f32),
            pltpu.VMEM((2, 1, rows3 + 2 * SUB, LANES), f32),
            pltpu.VMEM((count, tall, LANES), f32),
            pltpu.SemaphoreType.DMA((copies,)),
            pltpu.SemaphoreType.DMA((copies,)),
        ],
        compiler_params=pltpu.CompilerParams(
            collective_id=0, has_side_effects=True, vmem_limit_bytes=28 * 1024 * 1024
        ),
    )(
        velocity.reshape(3 * nz * nx, ny),
        old_tendency.reshape(3 * nz * nx, ny),
        obstacle.reshape(nz * nx, ny),
    )
    out = pl.pallas_call(
        functools.partial(finish, nz, nx),
        out_shape=(
            jax.ShapeDtypeStruct((3 * nz * nx, ny), f32),
            jax.ShapeDtypeStruct((nz * nx, ny), f32),
        ),
        in_specs=[pl.BlockSpec(memory_space=pltpu.VMEM)] * 4,
        out_specs=[pl.BlockSpec(memory_space=pltpu.VMEM)] * 2,
        compiler_params=pltpu.CompilerParams(vmem_limit_bytes=16 * 1024 * 1024),
    )(*parts, obstacle.reshape(nz * nx, ny))
    return out[0].reshape(3, nz, nx, ny), out[1].reshape(nz, nx, ny)


def solution(mesh):
    placed = (P(None, None, "gx", "gy"), P(None, None, "gx", "gy"), P(None, "gx", "gy"))
    return jax.shard_map(
        functools.partial(body, mesh.shape["gx"], mesh.shape["gy"]),
        mesh=mesh,
        in_specs=placed,
        out_specs=(P(None, None, "gx", "gy"), P(None, "gx", "gy")),
        check_vma=False,
    )
```

```python
import functools

import jax
import jax.numpy as jnp
from jax import lax
from jax.experimental import pallas as pl
from jax.experimental.pallas import tpu as pltpu
from jax.sharding import PartitionSpec as P

LEVELS = 3
SWEEPS = 2
COARSE_SWEEPS = 8
VISCOSITY = 0.1
TIME_STEP = 0.25
WEIGHT_NEW = 15.0 / 16.0
WEIGHT_OLD = -25.0 / 48.0
HELMHOLTZ = 0.0001

LANES = 128
SUB = 8
HALO_X = 8
HALO_Y = 8
HALO_1 = 8
MESH = pl.DeviceIdType.MESH


def iota2(shape, dim):
    return lax.broadcasted_iota(jnp.int32, shape, dim)


def mm(a, b):
    return jnp.dot(a, b, precision=lax.Precision.HIGHEST, preferred_element_type=jnp.float32)


class Level:
    def __init__(self, level, nz):
        self.nz = nz
        self.scale = 1.0 / float(4**level)
        lane = iota2((SUB, LANES), 1)
        row = iota2((SUB, LANES), 0)
        self.lane = lane
        self.row = row
        z = lane % nz
        self.not_top = z < nz - 1
        self.not_bottom = z > 0
        parity = (z + lane // nz + row) % 2
        self.colour = [parity == 0, parity == 1]
        edge = (z == 0) | (z == nz - 1)
        diag_in = HELMHOLTZ + 6.0 * self.scale
        diag_edge = HELMHOLTZ + 5.0 * self.scale
        self.diag = jnp.where(edge, diag_edge, diag_in).astype(jnp.float32)
        self.inv = jnp.where(edge, 1.0 / diag_edge, 1.0 / diag_in).astype(jnp.float32)
        self.take = jnp.where(
            edge, self.scale / diag_edge, self.scale / diag_in
        ).astype(jnp.float32)

    def x_plus(self, tiles, t):
        n = len(tiles)
        both = tiles[t] if n == 1 else jnp.where(self.lane < self.nz, tiles[(t + 1) % n], tiles[t])
        return pltpu.roll(both, LANES - self.nz, 1)

    def x_minus(self, tiles, t):
        n = len(tiles)
        last = self.lane >= LANES - self.nz
        both = tiles[t] if n == 1 else jnp.where(last, tiles[(t - 1) % n], tiles[t])
        return pltpu.roll(both, self.nz, 1)

    def y_plus(self, tile, following):
        return pltpu.roll(jnp.where(self.row == 0, following, tile), SUB - 1, 0)

    def y_minus(self, tile, previous):
        return pltpu.roll(jnp.where(self.row == SUB - 1, previous, tile), 1, 0)

    def z_plus(self, tile):
        return jnp.where(self.not_top, pltpu.roll(tile, LANES - 1, 1), 0.0)

    def z_minus(self, tile):
        return jnp.where(self.not_bottom, pltpu.roll(tile, 1, 1), 0.0)


def tile_of(t):
    return slice(t * LANES, (t + 1) * LANES)


def row_loop(tiles, unroll, body):
    while tiles % unroll:
        unroll -= 1

    def step(i, carry):
        for k in range(unroll):
            body(pl.multiple_of((i * unroll + k) * SUB, SUB))
        return carry

    lax.fori_loop(0, tiles // unroll, step, 0)


class Packed:
    def __init__(self, level, nz, n):
        self.n = n
        self.half = half = nz // 2
        self.scale = scale = 1.0 / float(4**level)
        lane, row = iota2((SUB, LANES), 1), iota2((SUB, LANES), 0)
        zh = lane % half
        diag_in, diag_edge = HELMHOLTZ + 6.0 * scale, HELMHOLTZ + 5.0 * scale
        odd = ((lane // half) * n + row) % 2 == 1
        self.odd = [odd, ~odd]
        self.up, self.down, self.diag, self.inv, self.take = [], [], [], [], []
        for v in (0, 1):
            up = self.odd[v] & (zh < half - 1)
            down = self.odd[1 - v] & (zh > 0)
            inside = up | down
            self.up.append(up)
            self.down.append(down)
            self.diag.append(jnp.where(inside, diag_in, diag_edge).astype(jnp.float32))
            self.inv.append(jnp.where(inside, 1.0 / diag_in, 1.0 / diag_edge).astype(jnp.float32))
            self.take.append(jnp.where(inside, scale / diag_in, scale / diag_edge).astype(jnp.float32))

    def totals(self, q, other, r):
        n = self.n
        here = [q[other, k, pl.ds(r, SUB), :] for k in range(n)]
        first = pltpu.roll(here[0], LANES - self.half, 1)
        last = pltpu.roll(here[n - 1], self.half, 1)
        out = []
        for k in range(n):
            v = (k + 1 - other) % 2
            b = here[k]
            east = here[k + 1] if k < n - 1 else first
            west = here[k - 1] if k > 0 else last
            north = q[other, k, pl.ds(r + 1, SUB), :]
            south = q[other, k, pl.ds(r - 1, SUB), :]
            z = jnp.where(
                self.up[v],
                pltpu.roll(b, LANES - 1, 1),
                jnp.where(self.down[v], pltpu.roll(b, 1, 1), 0.0),
            )
            out.append((east + west) + (north + south) + (b + z))
        return out

    def first(self, q, f, start, count, unroll):
        def body(i):
            for k in range(self.n):
                r = i + start
                q[0, k, pl.ds(r + SUB, SUB), :] = f[0, k, pl.ds(r, SUB), :] * self.inv[k % 2]

        row_loop(count, unroll, body)

    def half_sweep(self, q, f, c, start, count, unroll, wrap):
        if wrap:
            wrap_rows(q, 1 - c)

        def body(i):
            r = i + start
            total = self.totals(q, 1 - c, r + SUB)
            for k in range(self.n):
                v = (k + c) % 2
                q[c, k, pl.ds(r + SUB, SUB), :] = (
                    f[c, k, pl.ds(r, SUB), :] * self.inv[v] + total[k] * self.take[v]
                )

        row_loop(count, unroll, body)

    def presmooth(self, q, f, sweeps, count, unroll, wrap):
        self.first(q, f, 0, count, unroll)
        for k in range(1, 2 * sweeps):
            self.half_sweep(q, f, k % 2, 0, count, unroll, wrap)

    def postsmooth(self, q, f, start, count, unroll, wrap):
        for k in range(2 * SWEEPS):
            self.half_sweep(q, f, k % 2, start, count, unroll, wrap)

    def residual(self, q, f, out, start, count, unroll, wrap):
        if wrap:
            wrap_rows(q, 0)
            wrap_rows(q, 1)
        n = self.n

        def body(i):
            r = i + start
            parts = [None] * n
            for c in (0, 1):
                total = self.totals(q, 1 - c, r + SUB)
                for k in range(n):
                    v = (k + c) % 2
                    res = f[c, k, pl.ds(r, SUB), :] - (
                        self.diag[v] * q[c, k, pl.ds(r + SUB, SUB), :] - self.scale * total[k]
                    )
                    parts[k] = res if c == 0 else parts[k] + res
            if n == 1:
                out[0, pl.ds(i, SUB), :] = parts[0]
            else:
                for j in range(n // 2):
                    out[j, pl.ds(i, SUB), :] = parts[2 * j] + parts[2 * j + 1]

        row_loop(count, unroll, body)

    def colours(self, even, odd, k):
        rows = even.shape[0]
        odd_cell = jnp.concatenate([self.odd[k % 2]] * (rows // SUB), axis=0)
        return jnp.where(odd_cell, odd, even), jnp.where(odd_cell, even, odd)


def wrap_rows(q, c):
    rows = q.shape[2]
    for k in range(q.shape[1]):
        q[c, k, 0:SUB, :] = q[c, k, rows - 2 * SUB : rows - SUB, :]
        q[c, k, rows - SUB : rows, :] = q[c, k, SUB : 2 * SUB, :]


def pair_rows(ref, j, rows):
    return ref[j, pl.ds(0, rows, stride=2), :] + ref[j, pl.ds(1, rows, stride=2), :]


def twice_rows(value, pairs, j):
    rows = value.shape[0]
    pairs[j, pl.ds(0, rows, stride=2), :] = value
    pairs[j, pl.ds(1, rows, stride=2), :] = value


def matrix(rows, cols, weight, hit):
    i, o = iota2((rows, cols), 0), iota2((rows, cols), 1)
    return jnp.where(hit(i, o), weight, 0.0).astype(jnp.float32)


def kernel(
    nx_dev, ny_dev, nz, nx, ny,
    vel_hbm, old_hbm, obs_hbm, predn, pn, gn, wet,
    vel_in, old_in, obs_in,
    vel, old, fluid, edge, edge_in, pred,
    fe, fe_in, pe, pe_in, f0, fn, fs, f0q, p0, pk, pk_in, py_in, p1y_in,
    gath, f1, p1, m2, f2, p2, f3, p3, pairs, load_sem, send_sem, recv_sem,
):
    gx, gy = lax.axis_index("gx"), lax.axis_index("gy")

    def device(dx, dy):
        return (lax.rem(gx + dx + nx_dev, nx_dev), lax.rem(gy + dy + ny_dev, ny_dev))

    peers = [(d, 0) for d in range(1, nx_dev)] + [(0, d) for d in range(1, ny_dev)]
    peers += [(a, b) for a in range(1, nx_dev) for b in (-1, 1)]
    barrier = pltpu.get_barrier_semaphore()
    for dx, dy in peers:
        pl.semaphore_signal(barrier, inc=1, device_id=device(dx, dy), device_id_type=MESH)

    loads = [
        pltpu.make_async_copy(src, dst, load_sem.at[i])
        for i, (src, dst) in enumerate(((vel_hbm, vel_in), (old_hbm, old_in), (obs_hbm, obs_in)))
    ]
    for load in loads:
        load.start()

    number = [0]

    def send(src, dst, dx, dy):
        k = number[0]
        number[0] += 1
        copy = pltpu.make_async_remote_copy(
            src_ref=src, dst_ref=dst, send_sem=send_sem.at[k], recv_sem=recv_sem.at[k],
            device_id=device(dx, dy), device_id_type=MESH,
        )
        copy.start()
        return copy

    per = LANES // nz
    blocks = nx // per
    width = blocks * LANES
    lv0 = Level(0, nz)
    lane = lv0.lane

    def load_tile(ref, base, t):
        rows = [ref[pl.ds(base + t * per + i, nz, stride=nx), :] for i in range(per)]
        return jnp.concatenate(rows, axis=0).T

    loads[0].wait()
    for i in (0, 1):
        for c in range(3):
            edge[i, c * nz : (c + 1) * nz, :] = vel_in[
                pl.ds(c * nz * nx + (nx - 1 if i == 0 else 0), nz, stride=nx), :
            ]
    for c in range(3):
        for t in range(blocks):
            vel[c, SUB : SUB + ny, tile_of(t + 1)] = load_tile(vel_in, c * nz * nx, t)

    pltpu_wait = functools.partial(pl.semaphore_wait, barrier)
    pltpu_wait(len(peers))

    copies = [
        send(edge.at[0], edge_in.at[0], 1, 0),
        send(edge.at[1], edge_in.at[1], -1, 0),
        send(vel.at[:, ny : ny + SUB, LANES : LANES + width], vel.at[:, 0:SUB, LANES : LANES + width], 0, 1),
        send(
            vel.at[:, SUB : 2 * SUB, LANES : LANES + width],
            vel.at[:, SUB + ny : 2 * SUB + ny, LANES : LANES + width], 0, -1,
        ),
    ]

    loads[1].wait()
    loads[2].wait()
    for c in range(3):
        for t in range(blocks):
            old[c, :, tile_of(t)] = load_tile(old_in, c * nz * nx, t)
    for t in range(blocks):
        fluid[:, tile_of(t)] = (1 - load_tile(obs_in, 0, t)).astype(jnp.float32)
    for copy in copies:
        copy.wait()
    rest = jnp.zeros((LANES - 3 * nz, ny), jnp.float32)
    beside = [jnp.concatenate([edge_in[i], rest], axis=0).T for i in (0, 1)]
    for c in range(3):
        vel[c, SUB : SUB + ny, tile_of(0)] = pltpu.roll(beside[0], (LANES - nz - c * nz) % LANES, 1)
        vel[c, SUB : SUB + ny, tile_of(blocks + 1)] = pltpu.roll(beside[1], (-c * nz) % LANES, 1)

    def momentum(r):
        here = [
            [vel[c, pl.ds(r + SUB, SUB), tile_of(t)] for t in range(blocks + 2)] for c in range(3)
        ]
        for t in range(1, blocks + 1):
            cols = tile_of(t)
            wet = fluid[pl.ds(r, SUB), tile_of(t - 1)]
            for c in range(3):
                q = here[c][t]
                xp, xm = lv0.x_plus(here[c], t), lv0.x_minus(here[c], t)
                yp = lv0.y_plus(q, vel[c, pl.ds(r + 2 * SUB, SUB), cols])
                ym = lv0.y_minus(q, vel[c, pl.ds(r, SUB), cols])
                zp, zm = lv0.z_plus(q), lv0.z_minus(q)
                advect = 0.5 * (
                    here[0][t] * (xp - xm) + here[1][t] * (yp - ym) + here[2][t] * (zp - zm)
                )
                diffuse = xp + xm + yp + ym + zp + zm - 6.0 * q
                tendency = VISCOSITY * diffuse - advect
                pred[c, pl.ds(r + SUB, SUB), cols] = wet * (
                    q
                    + TIME_STEP
                    * (WEIGHT_NEW * tendency + WEIGHT_OLD * old[c, pl.ds(r, SUB), tile_of(t - 1)])
                )

    row_loop(ny // SUB, 16, momentum)

    inner = slice(LANES, LANES + width)
    own_rows = slice(SUB, SUB + ny)
    factor = 0.5 / TIME_STEP
    side = HALO_X // per
    none = jnp.zeros((SUB, LANES), jnp.float32)

    def source_of(r, t, whole):
        cols = tile_of(t)
        rows = pl.ds(r, SUB)
        first, last = r == (0 if whole else SUB), r == (SUB + ny if whole else ny)
        u = [pred[0, rows, tile_of(i)] for i in range(blocks + 2)] if whole else (
            [none] + [pred[0, rows, tile_of(i)] for i in range(1, blocks + 1)] + [none]
        )
        v, w = pred[1, rows, cols], pred[2, rows, cols]
        north = none if last else pred[1, pl.ds(r + SUB, SUB), cols]
        south = none if first else pred[1, pl.ds(r - SUB, SUB), cols]
        total = (
            (lv0.x_plus(u, t) - lv0.x_minus(u, t))
            + (lv0.y_plus(v, north) - lv0.y_minus(v, south))
            + (lv0.z_plus(w) - lv0.z_minus(w))
        )
        return total * (-factor)

    def turn_rows(ref, base, t, turned):
        for i in range(per):
            ref[pl.ds(base + t * per + i, nz, stride=nx), :] = turned[i * nz : (i + 1) * nz, :]

    copies = [
        send(pred.at[:, ny : ny + SUB, inner], pred.at[:, 0:SUB, inner], 0, 1),
        send(pred.at[:, SUB : 2 * SUB, inner], pred.at[:, SUB + ny : 2 * SUB + ny, inner], 0, -1),
    ]
    for dx in (1, -1):
        t = blocks if dx > 0 else 1
        far = tile_of(0 if dx > 0 else blocks + 1)
        for dy in (1, -1):
            rows = slice(ny, ny + SUB) if dy > 0 else slice(SUB, 2 * SUB)
            there = slice(0, SUB) if dy > 0 else slice(SUB + ny, 2 * SUB + ny)
            copies.append(send(pred.at[:, rows, tile_of(t)], pred.at[:, there, far], dx, dy))
            copies.append(send(pred.at[1, rows, tile_of(t)], pred.at[1, rows, far], dx, 0))
    for dx in (1, -1):
        i, t = (0, blocks) if dx > 0 else (1, 1)
        turned = pred[0, own_rows, tile_of(t)].T
        pe[i] = turned[LANES - nz : LANES, :] if dx > 0 else turned[0:nz, :]
        for r in range(0, ny, SUB):
            fe[i, r : r + SUB, :] = source_of(r + SUB, t, False)
        copies.append(send(fe.at[i], fe_in.at[i], dx, 0))
        copies.append(send(pe.at[i], pe_in.at[i], dx, 0))

    n0, half0 = per, nz // 2
    lv0p = Packed(0, nz, n0)
    tall0 = ny + 2 * HALO_Y
    blank = jnp.zeros((half0, ny), jnp.float32)
    group = iota2((SUB, LANES), 1) // half0
    slots = LANES // half0
    corners = [(a, b) for a in (1, -1) for b in (1, -1)]

    for c in range(3):
        for t in range(blocks):
            turn_rows(predn, c * nz * nx, t, pred[c, own_rows, tile_of(t + 1)].T)

    wet[...] = (1 - obs_in[...]).astype(jnp.float32)
    p0[...] = jnp.zeros(p0.shape, jnp.float32)
    p1[...] = jnp.zeros(p1.shape, jnp.float32)
    for copy in copies:
        copy.wait()

    blanks = jnp.zeros((LANES - nz, ny), jnp.float32)
    pred[0, own_rows, tile_of(0)] = jnp.concatenate([blanks, pe_in[0]], axis=0).T
    pred[0, own_rows, tile_of(blocks + 1)] = jnp.concatenate([pe_in[1], blanks], axis=0).T
    for r in range(0, tall0, SUB):
        strip = r == 0 or r == SUB + ny
        for t in range(blocks + 2):
            if strip or 1 <= t <= blocks:
                f0[r : r + SUB, tile_of(t)] = source_of(r, t, True)
                continue
            i = 0 if t == 0 else 1
            value = fe_in[i, r - SUB : r, :]
            near = pltpu.roll(
                pred[0, r : r + SUB, tile_of(1 if i == 0 else blocks)], LANES - nz if i == 0 else nz, 1
            )
            if i == 0:
                value = value - jnp.where(lane >= LANES - nz, factor * near, 0.0)
            else:
                value = value + jnp.where(lane < nz, factor * near, 0.0)
            if r == SUB:
                south = pltpu.roll(pred[1, 0:SUB, tile_of(t)], 1, 0)
                value = value + jnp.where(lv0.row == 0, factor * south, 0.0)
            if r == ny:
                north = pltpu.roll(pred[1, SUB + ny : 2 * SUB + ny, tile_of(t)], SUB - 1, 0)
                value = value - jnp.where(lv0.row == SUB - 1, factor * north, 0.0)
            f0[r : r + SUB, tile_of(t)] = value

    for t in range(blocks + 2):
        fn[t] = f0[own_rows, tile_of(t)].T
        strips = [f0[0:SUB, tile_of(t)], f0[SUB + ny : 2 * SUB + ny, tile_of(t)]]
        fs[t] = jnp.concatenate(strips + [jnp.zeros((LANES - 2 * SUB, LANES), jnp.float32)], axis=0).T

    def pack(ref, k, e):
        rows = [blank] * (side - 1)
        for t in range(blocks + 2):
            rows.append(ref[t, pl.ds(k * nz + e, half0, stride=2), :])
        rows += [blank] * (slots - len(rows))
        return jnp.concatenate(rows, axis=0).T

    for k in range(n0):
        both = lv0p.colours(pack(fn, k, 0), pack(fn, k, 1), k)
        ends = lv0p.colours(pack(fs, k, 0)[0 : 2 * SUB], pack(fs, k, 1)[0 : 2 * SUB], k)
        for c in (0, 1):
            f0q[c, k, HALO_Y : HALO_Y + ny, :] = both[c]
            f0q[c, k, 0:HALO_Y, :] = ends[c][0:SUB]
            f0q[c, k, HALO_Y + ny : tall0, :] = ends[c][SUB : 2 * SUB]

    tiles0 = tall0 // SUB
    lv0p.presmooth(p0, f0q, SWEEPS, tiles0, tiles0, False)
    lv0p.residual(p0, f0q, pairs, HALO_Y, ny // SUB, ny // SUB, False)

    own_x, nz1, half1 = nx // 2, nz // 2, nz // 4
    n1 = nx_dev * own_x * half1 // LANES
    lv1 = Packed(1, nz1, n1)
    wide = own_x // n1 * half1
    rows1 = ny // 2

    def down0(i, o):
        x = 2 * ((i % LANES) // half0 - side) + i // LANES
        z = i % half0
        place = ((z % 2) * n1 + x % n1) * wide + (x // n1) * half1 + z // 2
        return (x >= 0) & (x < own_x) & (place == o)

    sums = jnp.concatenate([pair_rows(pairs, j, rows1) for j in range(n0 // 2)], axis=1)
    gath[0, HALO_1 : HALO_1 + rows1, :] = mm(sums, matrix(LANES * (n0 // 2), LANES, 0.125, down0))
    body1 = slice(HALO_1, HALO_1 + rows1)
    copies = [send(gath.at[0, body1], gath.at[j, body1], nx_dev - j, 0) for j in range(1, nx_dev)]
    for j in range(nx_dev):
        copies.append(send(gath.at[0, rows1 : rows1 + HALO_1], gath.at[j, 0:HALO_1], nx_dev - j, 1))
        copies.append(
            send(gath.at[0, HALO_1 : 2 * HALO_1], gath.at[j, rows1 + HALO_1 : rows1 + 2 * HALO_1], nx_dev - j, -1)
        )

    own0 = SUB + HALO_Y
    for i in (0, 1):
        for r in range(0, ny, SUB):
            rows = slice(own0 + r, own0 + r + SUB)
            g, k = (side + blocks - 2, n0 - 1) if i == 0 else (side + 1, 0)
            out = pltpu.roll(p0[1, k, rows, :], ((n0 - g) * half0) % LANES, 1)
            g = side + blocks - 1 if i == 0 else side
            for m in range(n0):
                part = pltpu.roll(p0[1, m, rows, :], ((m - g) * half0) % LANES, 1)
                out = jnp.where(group == m, part, out)
            pk[i, r : r + SUB, :] = out
    for copy in copies:
        copy.wait()
    later = [
        send(p0.at[1, :, own0 + ny - SUB : own0 + ny, :], py_in.at[0], 0, 1),
        send(p0.at[1, :, own0 : own0 + SUB, :], py_in.at[1], 0, -1),
    ]
    for dx in (1, -1):
        i = 0 if dx > 0 else 1
        later.append(send(pk.at[i], pk_in.at[i, HALO_Y : HALO_Y + ny], dx, 0))
        later.append(send(pk.at[i, ny - SUB : ny], pk_in.at[i, 0:HALO_Y], dx, 1))
        later.append(send(pk.at[i, 0:SUB], pk_in.at[i, HALO_Y + ny : tall0], dx, -1))

    tall1 = rows1 + 2 * HALO_1
    source = iota2((SUB, LANES), 1) // wide

    def spread(r):
        parts = [gath[j, pl.ds(r, SUB), :] for j in range(nx_dev)]
        arr = []
        for m in range(2 * n1):
            out = pltpu.roll(parts[0], (-m * wide) % LANES, 1) if m else parts[0]
            for j in range(1, nx_dev):
                moved = pltpu.roll(parts[j], ((j - m) * wide) % LANES, 1) if j != m else parts[j]
                out = jnp.where(source == j, moved, out)
            arr.append(out)
        for k in range(n1):
            both = lv1.colours(arr[k], arr[n1 + k], k)
            f1[0, k, pl.ds(r, SUB), :] = both[0]
            f1[1, k, pl.ds(r, SUB), :] = both[1]

    tiles1 = tall1 // SUB
    row_loop(tiles1, tiles1, spread)
    lv1.presmooth(p1, f1, SWEEPS, tiles1, tiles1, False)
    lv1.residual(p1, f1, pairs, HALO_1, rows1 // SUB, rows1 // SUB, False)

    x2, nz2, half2 = nx_dev * nx // 4, nz // 4, nz // 8
    lanes2 = x2 * half2
    lv2 = Packed(2, nz2, 1)
    pieces = max(1, n1 // 2)
    own2 = ny // 4

    def down1(i, o):
        x = (i % LANES) // half1 * pieces + i // LANES
        z = i % half1
        return (z % 2) * lanes2 + x * half2 + z // 2 == o

    sums = jnp.concatenate([pair_rows(pairs, j, own2) for j in range(pieces)], axis=1)
    m2[0:own2, :] = mm(sums, matrix(LANES * pieces, 2 * lanes2, 0.125, down1))
    copies = [
        send(m2.at[0:own2, :], m2.at[j * own2 : (j + 1) * own2, :], 0, ny_dev - j) for j in range(1, ny_dev)
    ]
    own1 = SUB + HALO_1
    beyond = [
        send(p1.at[1, :, own1 + rows1 - HALO_1 : own1 + rows1, :], p1y_in.at[0], 0, 1),
        send(p1.at[1, :, own1 : own1 + HALO_1, :], p1y_in.at[1], 0, -1),
    ]
    for copy in copies:
        copy.wait()
    rows2 = ny_dev * own2
    low_half = iota2((SUB, LANES), 1) < LANES // 2

    def spread2(r):
        if lanes2 == LANES:
            even, odd = m2[pl.ds(r, SUB), 0:LANES], m2[pl.ds(r, SUB), LANES : 2 * LANES]
        else:
            both = m2[pl.ds(r, SUB), :]
            turned = pltpu.roll(both, LANES // 2, 1)
            even, odd = jnp.where(low_half, both, turned), jnp.where(low_half, turned, both)
        both = lv2.colours(even, odd, 0)
        f2[0, 0, pl.ds(r, SUB), :] = both[0]
        f2[1, 0, pl.ds(r, SUB), :] = both[1]

    row_loop(rows2 // SUB, 32, spread2)
    lv2.presmooth(p2, f2, SWEEPS, rows2 // SUB, 32, True)
    lv2.residual(p2, f2, pairs, 0, rows2 // SUB, 32, True)

    x3, half3 = x2 // 2, half2 // 2
    lv3 = Packed(3, nz2 // 2, 1)
    rows3 = rows2 // 2

    def down2(i, o):
        lane = o % LANES
        hit = (i < lanes2) & (i // half2 // 2 == (lane // half3) % x3)
        return hit & (i % half2 == 2 * (lane % half3) + o // LANES)

    down = mm(pair_rows(pairs, 0, rows3), matrix(LANES, 2 * LANES, 0.125, down2))
    both = lv3.colours(down[:, 0:LANES], down[:, LANES : 2 * LANES], 0)
    f3[0, 0] = both[0]
    f3[1, 0] = both[1]
    lv3.presmooth(p3, f3, COARSE_SWEEPS, rows3 // SUB, 16, True)

    def up3(i, o):
        lane = i % LANES
        hit = (lane < x3 * half3) & (lane // half3 == (o // half2) % x2 // 2)
        return hit & (2 * (lane % half3) + i // LANES == o % half2)

    inner3 = slice(SUB, SUB + rows3)
    both = lv3.colours(p3[0, 0, inner3, :], p3[1, 0, inner3, :], 0)
    twice_rows(mm(jnp.concatenate(both, axis=1), matrix(2 * LANES, LANES, 1.0, up3)), pairs, 0)
    p2[1, 0, SUB : SUB + rows2, :] += pairs[0, 0:rows2, :]
    lv2.postsmooth(p2, f2, 0, rows2 // SUB, 32, True)
    wrap_rows(p2, 0)
    wrap_rows(p2, 1)

    def up2(i, o):
        lane, to = i % LANES, o % LANES
        hit = (lane < lanes2) & (lane // half2 == (to // half1) * pieces + o // LANES)
        return hit & (2 * (lane % half2) + i // LANES == to % half1)

    first2 = SUB - HALO_1 // 2
    window = slice(first2, first2 + tall1 // 2)
    both = lv2.colours(p2[0, 0, window, :], p2[1, 0, window, :], 0)
    lift = mm(jnp.concatenate(both, axis=1), matrix(2 * LANES, LANES * pieces, 1.0, up2))
    for j in range(pieces):
        twice_rows(lift[:, tile_of(j)], pairs, j)
    for copy in beyond:
        copy.wait()
    for k in range(n1):
        p1[1, k, SUB : SUB + HALO_1, :] = p1y_in[0, k]
        p1[1, k, own1 + rows1 : own1 + rows1 + HALO_1, :] = p1y_in[1, k]
        p1[1, k, SUB : SUB + tall1, :] += pairs[k * pieces // n1, 0:tall1, :]
    lv1.postsmooth(p1, f1, 0, tiles1, tiles1, False)

    reach = side * n0 // 2
    wide_x = own_x + 2 * reach
    take = wide_x // n1 * half1
    off = -reach // n1 * half1
    first1 = SUB + HALO_1 - HALO_Y // 2
    window = slice(first1, first1 + tall0 // 2)
    halves = [[], []]
    for k in range(n1):
        both = lv1.colours(p1[0, k, window, :], p1[1, k, window, :], k)
        halves[0].append(both[0])
        halves[1].append(both[1])
    slot = iota2((tall0 // 2, LANES), 1) // take
    joined = []
    for e in (0, 1):
        out = None
        for k in range(n1):
            moved = pltpu.roll(halves[e][k], (k * take - off) % LANES, 1)
            out = moved if out is None else jnp.where(slot == k, moved, out)
        joined.append(out)

    def up1(i, o):
        lane, to = i % LANES, o % LANES
        x = (lane % take) // half1 * n1 + lane // take
        hit = (lane < take * n1) & (x == to // half0 * (n0 // 2) + o // LANES)
        return hit & (2 * (lane % half1) + i // LANES == to % half0)

    lift = mm(jnp.concatenate(joined, axis=1), matrix(2 * LANES, LANES * (n0 // 2), 1.0, up1))
    for j in range(n0 // 2):
        twice_rows(lift[:, tile_of(j)], pairs, j)
    for copy in later:
        copy.wait()
    for r in range(0, tall0, SUB):
        rows = slice(SUB + r, 2 * SUB + r)
        for k in range(n0):
            if r == 0 or r == HALO_Y + ny:
                value = py_in[0 if r == 0 else 1, k]
            else:
                value = p0[1, k, rows, :]
            for i in (0, 1):
                g = side - 1 if i == 0 else side + blocks
                part = pltpu.roll(pk_in[i, r : r + SUB, :], ((g - k) * half0) % LANES, 1)
                value = jnp.where(group == g, part, value)
                if k == (n0 - 1 if i == 0 else 0):
                    g = side - 2 if i == 0 else side + blocks + 1
                    part = pltpu.roll(pk_in[i, r : r + SUB, :], ((g - n0) * half0) % LANES, 1)
                    value = jnp.where(group == g, part, value)
            p0[1, k, rows, :] = value + pairs[k // 2, r : r + SUB, :]
    lv0p.postsmooth(p0, f0q, 0, tiles0, tiles0, False)

    low = SUB + HALO_Y
    body0 = slice(low, low + ny)
    ext = nx + 2 * HALO_X
    for k in range(n0):
        value = lv0p.colours(p0[0, k, body0, :], p0[1, k, body0, :], k)
        slope = [
            p0[1 - c, k, low + 1 : low + 1 + ny, :] - p0[1 - c, k, low - 1 : low - 1 + ny, :] for c in (0, 1)
        ]
        slope = lv0p.colours(slope[0], slope[1], k)
        for e in (0, 1):
            turned, sloped = value[e].T, slope[e].T
            for b in range(side - 1, side + blocks + 1):
                part = slice(b * half0, (b + 1) * half0)
                pn[pl.ds(e * ext + b * n0 + k, half0, stride=2 * ext), :] = turned[part, :]
                if side <= b < side + blocks:
                    gn[pl.ds(e * nx + (b - side) * n0 + k, half0, stride=2 * nx), :] = sloped[part, :]


def finish(nz, nx, predn, pn, gn, wet_in, cor_out, pre_out):
    ext = nx + 2 * HALO_X

    def correct(z):
        for h in range(nx // SUB):
            def cells(dz, dx):
                return pn[pl.ds((z + dz) * ext + HALO_X + h * SUB + dx, SUB), :]

            here = pl.ds(z * nx + h * SUB, SUB)
            pre_out[here, :] = cells(0, 0)
            wet = wet_in[here, :]
            above = cells(1, 0) if z < nz - 1 else 0.0
            below = cells(-1, 0) if z > 0 else 0.0
            slope = (cells(0, 1) - cells(0, -1), gn[here, :], above - below)
            for c in range(3):
                there = pl.ds(c * nz * nx + z * nx + h * SUB, SUB)
                cor_out[there, :] = wet * (predn[there, :] - (0.5 * TIME_STEP) * slope[c])

    for z in range(nz):
        correct(z)


def body(nx_dev, ny_dev, velocity, old_tendency, obstacle):
    _, nz, nx, ny = velocity.shape
    width = nx * nz
    per = LANES // nz
    blocks = nx // per
    tall0 = ny + 2 * HALO_Y
    n1 = nx_dev * (nx // 2) * (nz // 4) // LANES
    tall1 = ny // 2 + 2 * HALO_1
    rows2 = ny_dev * ny // 4
    rows3 = rows2 // 2
    wide2 = 2 * (nx_dev * nx // 4) * (nz // 8)
    tall = max(tall0, tall1, rows2)
    count = max(per // 2, n1 // 2, 1)
    copies = 4 + 14 + 8 + (nx_dev - 1) + 2 * nx_dev + (ny_dev - 1) + 2
    f32 = jnp.float32
    parts = pl.pallas_call(
        functools.partial(kernel, nx_dev, ny_dev, nz, nx, ny),
        out_shape=(
            jax.ShapeDtypeStruct((3 * nz * nx, ny), f32),
            jax.ShapeDtypeStruct((nz * (nx + 2 * HALO_X), ny), f32),
            jax.ShapeDtypeStruct((nz * nx, ny), f32),
            jax.ShapeDtypeStruct((nz * nx, ny), f32),
        ),
        in_specs=[pl.BlockSpec(memory_space=pltpu.HBM)] * 3,
        out_specs=[pl.BlockSpec(memory_space=pltpu.VMEM)] * 4,
        scratch_shapes=[
            pltpu.VMEM((3 * nz * nx, ny), f32),
            pltpu.VMEM((3 * nz * nx, ny), f32),
            pltpu.VMEM((nz * nx, ny), jnp.int32),
            pltpu.VMEM((3, ny + 2 * SUB, width + 2 * LANES), f32),
            pltpu.VMEM((3, ny, width), f32),
            pltpu.VMEM((ny, width), f32),
            pltpu.VMEM((2, 3 * nz, ny), f32),
            pltpu.VMEM((2, 3 * nz, ny), f32),
            pltpu.VMEM((3, ny + 2 * SUB, width + 2 * LANES), f32),
            pltpu.VMEM((2, ny, LANES), f32),
            pltpu.VMEM((2, ny, LANES), f32),
            pltpu.VMEM((2, nz, ny), f32),
            pltpu.VMEM((2, nz, ny), f32),
            pltpu.VMEM((tall0, width + 2 * LANES), f32),
            pltpu.VMEM((blocks + 2, LANES, ny), f32),
            pltpu.VMEM((blocks + 2, LANES, ny), f32),
            pltpu.VMEM((2, per, tall0, LANES), f32),
            pltpu.VMEM((2, per, tall0 + 2 * SUB, LANES), f32),
            pltpu.VMEM((2, ny, LANES), f32),
            pltpu.VMEM((2, tall0, LANES), f32),
            pltpu.VMEM((2, per, SUB, LANES), f32),
            pltpu.VMEM((2, n1, HALO_1, LANES), f32),
            pltpu.VMEM((nx_dev, tall1, LANES), f32),
            pltpu.VMEM((2, n1, tall1, LANES), f32),
            pltpu.VMEM((2, n1, tall1 + 2 * SUB, LANES), f32),
            pltpu.VMEM((rows2, wide2), f32),
            pltpu.VMEM((2, 1, rows2, LANES), f32),
            pltpu.VMEM((2, 1, rows2 + 2 * SUB, LANES), f32),
            pltpu.VMEM((2, 1, rows3, LANES), f32),
            pltpu.VMEM((2, 1, rows3 + 2 * SUB, LANES), f32),
            pltpu.VMEM((count, tall, LANES), f32),
            pltpu.SemaphoreType.DMA((3,)),
            pltpu.SemaphoreType.DMA((copies,)),
            pltpu.SemaphoreType.DMA((copies,)),
        ],
        compiler_params=pltpu.CompilerParams(
            collective_id=0, has_side_effects=True, vmem_limit_bytes=28 * 1024 * 1024
        ),
    )(
        pltpu.with_memory_space_constraint(velocity.reshape(3 * nz * nx, ny), pltpu.HBM),
        pltpu.with_memory_space_constraint(old_tendency.reshape(3 * nz * nx, ny), pltpu.HBM),
        pltpu.with_memory_space_constraint(obstacle.reshape(nz * nx, ny), pltpu.HBM),
    )
    out = pl.pallas_call(
        functools.partial(finish, nz, nx),
        out_shape=(
            jax.ShapeDtypeStruct((3 * nz * nx, ny), f32),
            jax.ShapeDtypeStruct((nz * nx, ny), f32),
        ),
        in_specs=[pl.BlockSpec(memory_space=pltpu.VMEM)] * 4,
        out_specs=[pl.BlockSpec(memory_space=pltpu.VMEM)] * 2,
        compiler_params=pltpu.CompilerParams(vmem_limit_bytes=16 * 1024 * 1024),
    )(*parts)
    return out[0].reshape(3, nz, nx, ny), out[1].reshape(nz, nx, ny)


def solution(mesh):
    placed = (P(None, None, "gx", "gy"), P(None, None, "gx", "gy"), P(None, "gx", "gy"))
    return jax.shard_map(
        functools.partial(body, mesh.shape["gx"], mesh.shape["gy"]),
        mesh=mesh,
        in_specs=placed,
        out_specs=(P(None, None, "gx", "gy"), P(None, "gx", "gy")),
        check_vma=False,
    )
```

```python
import functools

import jax
import jax.numpy as jnp
from jax import lax
from jax.experimental import pallas as pl
from jax.experimental.pallas import tpu as pltpu
from jax.sharding import PartitionSpec as P

LEVELS = 3
SWEEPS = 2
COARSE_SWEEPS = 8
VISCOSITY = 0.1
TIME_STEP = 0.25
WEIGHT_NEW = 15.0 / 16.0
WEIGHT_OLD = -25.0 / 48.0
HELMHOLTZ = 0.0001

LANES = 128
SUB = 8
HALO_X = 8
HALO_Y = 8
HALO_1 = 8
MESH = pl.DeviceIdType.MESH


def iota2(shape, dim):
    return lax.broadcasted_iota(jnp.int32, shape, dim)


def mm(a, b):
    return jnp.dot(a, b, precision=lax.Precision.HIGHEST, preferred_element_type=jnp.float32)


class Level:
    def __init__(self, level, nz):
        self.nz = nz
        self.scale = 1.0 / float(4**level)
        lane = iota2((SUB, LANES), 1)
        row = iota2((SUB, LANES), 0)
        self.lane = lane
        self.row = row
        z = lane % nz
        self.not_top = z < nz - 1
        self.not_bottom = z > 0
        parity = (z + lane // nz + row) % 2
        self.colour = [parity == 0, parity == 1]
        edge = (z == 0) | (z == nz - 1)
        diag_in = HELMHOLTZ + 6.0 * self.scale
        diag_edge = HELMHOLTZ + 5.0 * self.scale
        self.diag = jnp.where(edge, diag_edge, diag_in).astype(jnp.float32)
        self.inv = jnp.where(edge, 1.0 / diag_edge, 1.0 / diag_in).astype(jnp.float32)
        self.take = jnp.where(
            edge, self.scale / diag_edge, self.scale / diag_in
        ).astype(jnp.float32)

    def x_plus(self, tiles, t):
        n = len(tiles)
        both = tiles[t] if n == 1 else jnp.where(self.lane < self.nz, tiles[(t + 1) % n], tiles[t])
        return pltpu.roll(both, LANES - self.nz, 1)

    def x_minus(self, tiles, t):
        n = len(tiles)
        last = self.lane >= LANES - self.nz
        both = tiles[t] if n == 1 else jnp.where(last, tiles[(t - 1) % n], tiles[t])
        return pltpu.roll(both, self.nz, 1)

    def y_plus(self, tile, following):
        return pltpu.roll(jnp.where(self.row == 0, following, tile), SUB - 1, 0)

    def y_minus(self, tile, previous):
        return pltpu.roll(jnp.where(self.row == SUB - 1, previous, tile), 1, 0)

    def z_plus(self, tile):
        return jnp.where(self.not_top, pltpu.roll(tile, LANES - 1, 1), 0.0)

    def z_minus(self, tile):
        return jnp.where(self.not_bottom, pltpu.roll(tile, 1, 1), 0.0)


def tile_of(t):
    return slice(t * LANES, (t + 1) * LANES)


def row_loop(tiles, unroll, body):
    while tiles % unroll:
        unroll -= 1

    def step(i, carry):
        for k in range(unroll):
            body(pl.multiple_of((i * unroll + k) * SUB, SUB))
        return carry

    lax.fori_loop(0, tiles // unroll, step, 0)


class Packed:
    def __init__(self, level, nz, n):
        self.n = n
        self.half = half = nz // 2
        self.scale = scale = 1.0 / float(4**level)
        lane, row = iota2((SUB, LANES), 1), iota2((SUB, LANES), 0)
        zh = lane % half
        diag_in, diag_edge = HELMHOLTZ + 6.0 * scale, HELMHOLTZ + 5.0 * scale
        odd = ((lane // half) * n + row) % 2 == 1
        self.odd = [odd, ~odd]
        self.up, self.down, self.diag, self.inv, self.take = [], [], [], [], []
        for v in (0, 1):
            up = self.odd[v] & (zh < half - 1)
            down = self.odd[1 - v] & (zh > 0)
            inside = up | down
            self.up.append(up)
            self.down.append(down)
            self.diag.append(jnp.where(inside, diag_in, diag_edge).astype(jnp.float32))
            self.inv.append(jnp.where(inside, 1.0 / diag_in, 1.0 / diag_edge).astype(jnp.float32))
            self.take.append(jnp.where(inside, scale / diag_in, scale / diag_edge).astype(jnp.float32))

    def totals(self, q, other, r):
        n = self.n
        here = [q[other, k, pl.ds(r, SUB), :] for k in range(n)]
        first = pltpu.roll(here[0], LANES - self.half, 1)
        last = pltpu.roll(here[n - 1], self.half, 1)
        out = []
        for k in range(n):
            v = (k + 1 - other) % 2
            b = here[k]
            east = here[k + 1] if k < n - 1 else first
            west = here[k - 1] if k > 0 else last
            north = q[other, k, pl.ds(r + 1, SUB), :]
            south = q[other, k, pl.ds(r - 1, SUB), :]
            z = jnp.where(
                self.up[v],
                pltpu.roll(b, LANES - 1, 1),
                jnp.where(self.down[v], pltpu.roll(b, 1, 1), 0.0),
            )
            out.append((east + west) + (north + south) + (b + z))
        return out

    def first(self, q, f, start, count, unroll):
        def body(i):
            for k in range(self.n):
                r = i + start
                q[0, k, pl.ds(r + SUB, SUB), :] = f[0, k, pl.ds(r, SUB), :] * self.inv[k % 2]

        row_loop(count, unroll, body)

    def half_sweep(self, q, f, c, start, count, unroll, wrap):
        if wrap:
            wrap_rows(q, 1 - c)

        def body(i):
            r = i + start
            total = self.totals(q, 1 - c, r + SUB)
            for k in range(self.n):
                v = (k + c) % 2
                q[c, k, pl.ds(r + SUB, SUB), :] = (
                    f[c, k, pl.ds(r, SUB), :] * self.inv[v] + total[k] * self.take[v]
                )

        row_loop(count, unroll, body)

    def presmooth(self, q, f, sweeps, count, unroll, wrap):
        self.first(q, f, 0, count, unroll)
        for k in range(1, 2 * sweeps):
            self.half_sweep(q, f, k % 2, 0, count, unroll, wrap)

    def postsmooth(self, q, f, start, count, unroll, wrap):
        for k in range(2 * SWEEPS):
            self.half_sweep(q, f, k % 2, start, count, unroll, wrap)

    def residual(self, q, f, out, start, count, unroll, wrap):
        if wrap:
            wrap_rows(q, 0)
            wrap_rows(q, 1)
        n = self.n

        def body(i):
            r = i + start
            parts = [None] * n
            for c in (0, 1):
                total = self.totals(q, 1 - c, r + SUB)
                for k in range(n):
                    v = (k + c) % 2
                    res = f[c, k, pl.ds(r, SUB), :] - (
                        self.diag[v] * q[c, k, pl.ds(r + SUB, SUB), :] - self.scale * total[k]
                    )
                    parts[k] = res if c == 0 else parts[k] + res
            if n == 1:
                out[0, pl.ds(i, SUB), :] = parts[0]
            else:
                for j in range(n // 2):
                    out[j, pl.ds(i, SUB), :] = parts[2 * j] + parts[2 * j + 1]

        row_loop(count, unroll, body)

    def colours(self, even, odd, k):
        rows = even.shape[0]
        odd_cell = jnp.concatenate([self.odd[k % 2]] * (rows // SUB), axis=0)
        return jnp.where(odd_cell, odd, even), jnp.where(odd_cell, even, odd)


def wrap_rows(q, c):
    rows = q.shape[2]
    for k in range(q.shape[1]):
        q[c, k, 0:SUB, :] = q[c, k, rows - 2 * SUB : rows - SUB, :]
        q[c, k, rows - SUB : rows, :] = q[c, k, SUB : 2 * SUB, :]


def pair_rows(ref, j, rows):
    return ref[j, pl.ds(0, rows, stride=2), :] + ref[j, pl.ds(1, rows, stride=2), :]


def twice_rows(value, pairs, j):
    rows = value.shape[0]
    pairs[j, pl.ds(0, rows, stride=2), :] = value
    pairs[j, pl.ds(1, rows, stride=2), :] = value


def matrix(rows, cols, weight, hit):
    i, o = iota2((rows, cols), 0), iota2((rows, cols), 1)
    return jnp.where(hit(i, o), weight, 0.0).astype(jnp.float32)


def kernel(
    nx_dev, ny_dev, nz, nx, ny,
    vel_hbm, old_hbm, obs_hbm, predn, pn, gn, wet,
    vel_in, old_in, obs_in,
    vel, old, fluid, edge, edge_in, pred,
    fe, fe_in, pe, pe_in, f0, fn, fs, f0q, p0, pk, pk_in, py_in, p1y_in,
    gath, f1, p1, m2, f2, p2, f3, p3, pairs, load_sem, send_sem, recv_sem,
):
    gx, gy = lax.axis_index("gx"), lax.axis_index("gy")

    def device(dx, dy):
        return (lax.rem(gx + dx + nx_dev, nx_dev), lax.rem(gy + dy + ny_dev, ny_dev))

    peers = [(d, 0) for d in range(1, nx_dev)] + [(0, d) for d in range(1, ny_dev)]
    peers += [(a, b) for a in range(1, nx_dev) for b in (-1, 1)]
    barrier = pltpu.get_barrier_semaphore()
    for dx, dy in peers:
        pl.semaphore_signal(barrier, inc=1, device_id=device(dx, dy), device_id_type=MESH)

    loads = [
        pltpu.make_async_copy(src, dst, load_sem.at[i])
        for i, (src, dst) in enumerate(((vel_hbm, vel_in), (old_hbm, old_in), (obs_hbm, obs_in)))
    ]
    for load in loads:
        load.start()

    number = [0]

    def send(src, dst, dx, dy):
        k = number[0]
        number[0] += 1
        copy = pltpu.make_async_remote_copy(
            src_ref=src, dst_ref=dst, send_sem=send_sem.at[k], recv_sem=recv_sem.at[k],
            device_id=device(dx, dy), device_id_type=MESH,
        )
        copy.start()
        return copy

    per = LANES // nz
    blocks = nx // per
    width = blocks * LANES
    lv0 = Level(0, nz)
    lane = lv0.lane

    def load_tile(ref, base, t):
        rows = [ref[pl.ds(base + t * per + i, nz, stride=nx), :] for i in range(per)]
        return jnp.concatenate(rows, axis=0).T

    loads[0].wait()
    for i in (0, 1):
        for c in range(3):
            edge[i, c * nz : (c + 1) * nz, :] = vel_in[
                pl.ds(c * nz * nx + (nx - 1 if i == 0 else 0), nz, stride=nx), :
            ]
    for c in range(3):
        for t in range(blocks):
            vel[c, SUB : SUB + ny, tile_of(t + 1)] = load_tile(vel_in, c * nz * nx, t)

    pltpu_wait = functools.partial(pl.semaphore_wait, barrier)
    pltpu_wait(len(peers))

    copies = [
        send(edge.at[0], edge_in.at[0], 1, 0),
        send(edge.at[1], edge_in.at[1], -1, 0),
        send(vel.at[:, ny : ny + SUB, LANES : LANES + width], vel.at[:, 0:SUB, LANES : LANES + width], 0, 1),
        send(
            vel.at[:, SUB : 2 * SUB, LANES : LANES + width],
            vel.at[:, SUB + ny : 2 * SUB + ny, LANES : LANES + width], 0, -1,
        ),
    ]

    loads[1].wait()
    loads[2].wait()
    for c in range(3):
        for t in range(blocks):
            old[c, :, tile_of(t)] = load_tile(old_in, c * nz * nx, t)
    for t in range(blocks):
        fluid[:, tile_of(t)] = (1 - load_tile(obs_in, 0, t)).astype(jnp.float32)
    for copy in copies:
        copy.wait()
    rest = jnp.zeros((LANES - 3 * nz, ny), jnp.float32)
    beside = [jnp.concatenate([edge_in[i], rest], axis=0).T for i in (0, 1)]
    for c in range(3):
        vel[c, SUB : SUB + ny, tile_of(0)] = pltpu.roll(beside[0], (LANES - nz - c * nz) % LANES, 1)
        vel[c, SUB : SUB + ny, tile_of(blocks + 1)] = pltpu.roll(beside[1], (-c * nz) % LANES, 1)

    def momentum(r):
        here = [
            [vel[c, pl.ds(r + SUB, SUB), tile_of(t)] for t in range(blocks + 2)] for c in range(3)
        ]
        for t in range(1, blocks + 1):
            cols = tile_of(t)
            wet = fluid[pl.ds(r, SUB), tile_of(t - 1)]
            for c in range(3):
                q = here[c][t]
                xp, xm = lv0.x_plus(here[c], t), lv0.x_minus(here[c], t)
                yp = lv0.y_plus(q, vel[c, pl.ds(r + 2 * SUB, SUB), cols])
                ym = lv0.y_minus(q, vel[c, pl.ds(r, SUB), cols])
                zp, zm = lv0.z_plus(q), lv0.z_minus(q)
                advect = 0.5 * (
                    here[0][t] * (xp - xm) + here[1][t] * (yp - ym) + here[2][t] * (zp - zm)
                )
                diffuse = xp + xm + yp + ym + zp + zm - 6.0 * q
                tendency = VISCOSITY * diffuse - advect
                pred[c, pl.ds(r + SUB, SUB), cols] = wet * (
                    q
                    + TIME_STEP
                    * (WEIGHT_NEW * tendency + WEIGHT_OLD * old[c, pl.ds(r, SUB), tile_of(t - 1)])
                )

    row_loop(ny // SUB, 16, momentum)

    inner = slice(LANES, LANES + width)
    own_rows = slice(SUB, SUB + ny)
    factor = 0.5 / TIME_STEP
    side = HALO_X // per
    none = jnp.zeros((SUB, LANES), jnp.float32)

    def source_of(r, t, whole):
        cols = tile_of(t)
        rows = pl.ds(r, SUB)
        first, last = r == (0 if whole else SUB), r == (SUB + ny if whole else ny)
        u = [pred[0, rows, tile_of(i)] for i in range(blocks + 2)] if whole else (
            [none] + [pred[0, rows, tile_of(i)] for i in range(1, blocks + 1)] + [none]
        )
        v, w = pred[1, rows, cols], pred[2, rows, cols]
        north = none if last else pred[1, pl.ds(r + SUB, SUB), cols]
        south = none if first else pred[1, pl.ds(r - SUB, SUB), cols]
        total = (
            (lv0.x_plus(u, t) - lv0.x_minus(u, t))
            + (lv0.y_plus(v, north) - lv0.y_minus(v, south))
            + (lv0.z_plus(w) - lv0.z_minus(w))
        )
        return total * (-factor)

    def turn_rows(ref, base, t, turned):
        for i in range(per):
            ref[pl.ds(base + t * per + i, nz, stride=nx), :] = turned[i * nz : (i + 1) * nz, :]

    copies = [
        send(pred.at[:, ny : ny + SUB, inner], pred.at[:, 0:SUB, inner], 0, 1),
        send(pred.at[:, SUB : 2 * SUB, inner], pred.at[:, SUB + ny : 2 * SUB + ny, inner], 0, -1),
    ]
    for dx in (1, -1):
        t = blocks if dx > 0 else 1
        far = tile_of(0 if dx > 0 else blocks + 1)
        for dy in (1, -1):
            rows = slice(ny, ny + SUB) if dy > 0 else slice(SUB, 2 * SUB)
            there = slice(0, SUB) if dy > 0 else slice(SUB + ny, 2 * SUB + ny)
            copies.append(send(pred.at[:, rows, tile_of(t)], pred.at[:, there, far], dx, dy))
            copies.append(send(pred.at[1, rows, tile_of(t)], pred.at[1, rows, far], dx, 0))
    for dx in (1, -1):
        i, t = (0, blocks) if dx > 0 else (1, 1)
        turned = pred[0, own_rows, tile_of(t)].T
        pe[i] = turned[LANES - nz : LANES, :] if dx > 0 else turned[0:nz, :]
        for r in range(0, ny, SUB):
            fe[i, r : r + SUB, :] = source_of(r + SUB, t, False)
        copies.append(send(fe.at[i], fe_in.at[i], dx, 0))
        copies.append(send(pe.at[i], pe_in.at[i], dx, 0))

    n0, half0 = per, nz // 2
    lv0p = Packed(0, nz, n0)
    tall0 = ny + 2 * HALO_Y
    blank = jnp.zeros((half0, ny), jnp.float32)
    group = iota2((SUB, LANES), 1) // half0
    slots = LANES // half0
    corners = [(a, b) for a in (1, -1) for b in (1, -1)]

    for c in range(3):
        for t in range(blocks):
            turn_rows(predn, c * nz * nx, t, pred[c, own_rows, tile_of(t + 1)].T)

    for r in range(2 * SUB, ny, SUB):
        for t in range(2, blocks):
            f0[r : r + SUB, tile_of(t)] = source_of(r, t, True)
    wet[...] = (1 - obs_in[...]).astype(jnp.float32)
    p0[...] = jnp.zeros(p0.shape, jnp.float32)
    p1[...] = jnp.zeros(p1.shape, jnp.float32)
    for copy in copies:
        copy.wait()

    blanks = jnp.zeros((LANES - nz, ny), jnp.float32)
    pred[0, own_rows, tile_of(0)] = jnp.concatenate([blanks, pe_in[0]], axis=0).T
    pred[0, own_rows, tile_of(blocks + 1)] = jnp.concatenate([pe_in[1], blanks], axis=0).T
    for r in range(0, tall0, SUB):
        strip = r == 0 or r == SUB + ny
        for t in range(blocks + 2):
            if 2 * SUB <= r < ny and 2 <= t < blocks:
                continue
            if strip or 1 <= t <= blocks:
                f0[r : r + SUB, tile_of(t)] = source_of(r, t, True)
                continue
            i = 0 if t == 0 else 1
            value = fe_in[i, r - SUB : r, :]
            near = pltpu.roll(
                pred[0, r : r + SUB, tile_of(1 if i == 0 else blocks)], LANES - nz if i == 0 else nz, 1
            )
            if i == 0:
                value = value - jnp.where(lane >= LANES - nz, factor * near, 0.0)
            else:
                value = value + jnp.where(lane < nz, factor * near, 0.0)
            if r == SUB:
                south = pltpu.roll(pred[1, 0:SUB, tile_of(t)], 1, 0)
                value = value + jnp.where(lv0.row == 0, factor * south, 0.0)
            if r == ny:
                north = pltpu.roll(pred[1, SUB + ny : 2 * SUB + ny, tile_of(t)], SUB - 1, 0)
                value = value - jnp.where(lv0.row == SUB - 1, factor * north, 0.0)
            f0[r : r + SUB, tile_of(t)] = value

    for t in range(blocks + 2):
        fn[t] = f0[own_rows, tile_of(t)].T
        strips = [f0[0:SUB, tile_of(t)], f0[SUB + ny : 2 * SUB + ny, tile_of(t)]]
        fs[t] = jnp.concatenate(strips + [jnp.zeros((LANES - 2 * SUB, LANES), jnp.float32)], axis=0).T

    def pack(ref, k, e):
        rows = [blank] * (side - 1)
        for t in range(blocks + 2):
            rows.append(ref[t, pl.ds(k * nz + e, half0, stride=2), :])
        rows += [blank] * (slots - len(rows))
        return jnp.concatenate(rows, axis=0).T

    for k in range(n0):
        both = lv0p.colours(pack(fn, k, 0), pack(fn, k, 1), k)
        ends = lv0p.colours(pack(fs, k, 0)[0 : 2 * SUB], pack(fs, k, 1)[0 : 2 * SUB], k)
        for c in (0, 1):
            f0q[c, k, HALO_Y : HALO_Y + ny, :] = both[c]
            f0q[c, k, 0:HALO_Y, :] = ends[c][0:SUB]
            f0q[c, k, HALO_Y + ny : tall0, :] = ends[c][SUB : 2 * SUB]

    tiles0 = tall0 // SUB
    lv0p.presmooth(p0, f0q, SWEEPS, tiles0, tiles0, False)
    lv0p.residual(p0, f0q, pairs, HALO_Y, ny // SUB, ny // SUB, False)

    own_x, nz1, half1 = nx // 2, nz // 2, nz // 4
    n1 = nx_dev * own_x * half1 // LANES
    lv1 = Packed(1, nz1, n1)
    wide = own_x // n1 * half1
    rows1 = ny // 2

    def down0(i, o):
        x = 2 * ((i % LANES) // half0 - side) + i // LANES
        z = i % half0
        place = ((z % 2) * n1 + x % n1) * wide + (x // n1) * half1 + z // 2
        return (x >= 0) & (x < own_x) & (place == o)

    sums = jnp.concatenate([pair_rows(pairs, j, rows1) for j in range(n0 // 2)], axis=1)
    gath[0, HALO_1 : HALO_1 + rows1, :] = mm(sums, matrix(LANES * (n0 // 2), LANES, 0.125, down0))
    body1 = slice(HALO_1, HALO_1 + rows1)
    copies = [send(gath.at[0, body1], gath.at[j, body1], nx_dev - j, 0) for j in range(1, nx_dev)]
    for j in range(nx_dev):
        copies.append(send(gath.at[0, rows1 : rows1 + HALO_1], gath.at[j, 0:HALO_1], nx_dev - j, 1))
        copies.append(
            send(gath.at[0, HALO_1 : 2 * HALO_1], gath.at[j, rows1 + HALO_1 : rows1 + 2 * HALO_1], nx_dev - j, -1)
        )

    own0 = SUB + HALO_Y
    for i in (0, 1):
        for r in range(0, ny, SUB):
            rows = slice(own0 + r, own0 + r + SUB)
            g, k = (side + blocks - 2, n0 - 1) if i == 0 else (side + 1, 0)
            out = pltpu.roll(p0[1, k, rows, :], ((n0 - g) * half0) % LANES, 1)
            g = side + blocks - 1 if i == 0 else side
            for m in range(n0):
                part = pltpu.roll(p0[1, m, rows, :], ((m - g) * half0) % LANES, 1)
                out = jnp.where(group == m, part, out)
            pk[i, r : r + SUB, :] = out
    for copy in copies:
        copy.wait()
    later = [
        send(p0.at[1, :, own0 + ny - SUB : own0 + ny, :], py_in.at[0], 0, 1),
        send(p0.at[1, :, own0 : own0 + SUB, :], py_in.at[1], 0, -1),
    ]
    for dx in (1, -1):
        i = 0 if dx > 0 else 1
        later.append(send(pk.at[i], pk_in.at[i, HALO_Y : HALO_Y + ny], dx, 0))
        later.append(send(pk.at[i, ny - SUB : ny], pk_in.at[i, 0:HALO_Y], dx, 1))
        later.append(send(pk.at[i, 0:SUB], pk_in.at[i, HALO_Y + ny : tall0], dx, -1))

    tall1 = rows1 + 2 * HALO_1
    source = iota2((SUB, LANES), 1) // wide

    def spread(r):
        parts = [gath[j, pl.ds(r, SUB), :] for j in range(nx_dev)]
        arr = []
        for m in range(2 * n1):
            out = pltpu.roll(parts[0], (-m * wide) % LANES, 1) if m else parts[0]
            for j in range(1, nx_dev):
                moved = pltpu.roll(parts[j], ((j - m) * wide) % LANES, 1) if j != m else parts[j]
                out = jnp.where(source == j, moved, out)
            arr.append(out)
        for k in range(n1):
            both = lv1.colours(arr[k], arr[n1 + k], k)
            f1[0, k, pl.ds(r, SUB), :] = both[0]
            f1[1, k, pl.ds(r, SUB), :] = both[1]

    tiles1 = tall1 // SUB
    row_loop(tiles1, tiles1, spread)
    lv1.presmooth(p1, f1, SWEEPS, tiles1, tiles1, False)
    lv1.residual(p1, f1, pairs, HALO_1, rows1 // SUB, rows1 // SUB, False)

    x2, nz2, half2 = nx_dev * nx // 4, nz // 4, nz // 8
    lanes2 = x2 * half2
    lv2 = Packed(2, nz2, 1)
    pieces = max(1, n1 // 2)
    own2 = ny // 4

    def down1(i, o):
        x = (i % LANES) // half1 * pieces + i // LANES
        z = i % half1
        return (z % 2) * lanes2 + x * half2 + z // 2 == o

    sums = jnp.concatenate([pair_rows(pairs, j, own2) for j in range(pieces)], axis=1)
    m2[0:own2, :] = mm(sums, matrix(LANES * pieces, 2 * lanes2, 0.125, down1))
    copies = [
        send(m2.at[0:own2, :], m2.at[j * own2 : (j + 1) * own2, :], 0, ny_dev - j) for j in range(1, ny_dev)
    ]
    own1 = SUB + HALO_1
    beyond = [
        send(p1.at[1, :, own1 + rows1 - HALO_1 : own1 + rows1, :], p1y_in.at[0], 0, 1),
        send(p1.at[1, :, own1 : own1 + HALO_1, :], p1y_in.at[1], 0, -1),
    ]
    for copy in copies:
        copy.wait()
    rows2 = ny_dev * own2
    low_half = iota2((SUB, LANES), 1) < LANES // 2

    def spread2(r):
        if lanes2 == LANES:
            even, odd = m2[pl.ds(r, SUB), 0:LANES], m2[pl.ds(r, SUB), LANES : 2 * LANES]
        else:
            both = m2[pl.ds(r, SUB), :]
            turned = pltpu.roll(both, LANES // 2, 1)
            even, odd = jnp.where(low_half, both, turned), jnp.where(low_half, turned, both)
        both = lv2.colours(even, odd, 0)
        f2[0, 0, pl.ds(r, SUB), :] = both[0]
        f2[1, 0, pl.ds(r, SUB), :] = both[1]

    row_loop(rows2 // SUB, 32, spread2)
    lv2.presmooth(p2, f2, SWEEPS, rows2 // SUB, 32, True)
    lv2.residual(p2, f2, pairs, 0, rows2 // SUB, 32, True)

    x3, half3 = x2 // 2, half2 // 2
    lv3 = Packed(3, nz2 // 2, 1)
    rows3 = rows2 // 2

    def down2(i, o):
        lane = o % LANES
        hit = (i < lanes2) & (i // half2 // 2 == (lane // half3) % x3)
        return hit & (i % half2 == 2 * (lane % half3) + o // LANES)

    down = mm(pair_rows(pairs, 0, rows3), matrix(LANES, 2 * LANES, 0.125, down2))
    both = lv3.colours(down[:, 0:LANES], down[:, LANES : 2 * LANES], 0)
    f3[0, 0] = both[0]
    f3[1, 0] = both[1]
    lv3.presmooth(p3, f3, COARSE_SWEEPS, rows3 // SUB, 16, True)

    def up3(i, o):
        lane = i % LANES
        hit = (lane < x3 * half3) & (lane // half3 == (o // half2) % x2 // 2)
        return hit & (2 * (lane % half3) + i // LANES == o % half2)

    inner3 = slice(SUB, SUB + rows3)
    both = lv3.colours(p3[0, 0, inner3, :], p3[1, 0, inner3, :], 0)
    twice_rows(mm(jnp.concatenate(both, axis=1), matrix(2 * LANES, LANES, 1.0, up3)), pairs, 0)
    p2[1, 0, SUB : SUB + rows2, :] += pairs[0, 0:rows2, :]
    lv2.postsmooth(p2, f2, 0, rows2 // SUB, 32, True)
    wrap_rows(p2, 0)
    wrap_rows(p2, 1)

    def up2(i, o):
        lane, to = i % LANES, o % LANES
        hit = (lane < lanes2) & (lane // half2 == (to // half1) * pieces + o // LANES)
        return hit & (2 * (lane % half2) + i // LANES == to % half1)

    first2 = SUB - HALO_1 // 2
    window = slice(first2, first2 + tall1 // 2)
    both = lv2.colours(p2[0, 0, window, :], p2[1, 0, window, :], 0)
    lift = mm(jnp.concatenate(both, axis=1), matrix(2 * LANES, LANES * pieces, 1.0, up2))
    for j in range(pieces):
        twice_rows(lift[:, tile_of(j)], pairs, j)
    for copy in beyond:
        copy.wait()
    for k in range(n1):
        p1[1, k, SUB : SUB + HALO_1, :] = p1y_in[0, k]
        p1[1, k, own1 + rows1 : own1 + rows1 + HALO_1, :] = p1y_in[1, k]
        p1[1, k, SUB : SUB + tall1, :] += pairs[k * pieces // n1, 0:tall1, :]
    lv1.postsmooth(p1, f1, 0, tiles1, tiles1, False)

    reach = side * n0 // 2
    wide_x = own_x + 2 * reach
    take = wide_x // n1 * half1
    off = -reach // n1 * half1
    first1 = SUB + HALO_1 - HALO_Y // 2
    window = slice(first1, first1 + tall0 // 2)
    halves = [[], []]
    for k in range(n1):
        both = lv1.colours(p1[0, k, window, :], p1[1, k, window, :], k)
        halves[0].append(both[0])
        halves[1].append(both[1])
    slot = iota2((tall0 // 2, LANES), 1) // take
    joined = []
    for e in (0, 1):
        out = None
        for k in range(n1):
            moved = pltpu.roll(halves[e][k], (k * take - off) % LANES, 1)
            out = moved if out is None else jnp.where(slot == k, moved, out)
        joined.append(out)

    def up1(i, o):
        lane, to = i % LANES, o % LANES
        x = (lane % take) // half1 * n1 + lane // take
        hit = (lane < take * n1) & (x == to // half0 * (n0 // 2) + o // LANES)
        return hit & (2 * (lane % half1) + i // LANES == to % half0)

    lift = mm(jnp.concatenate(joined, axis=1), matrix(2 * LANES, LANES * (n0 // 2), 1.0, up1))
    for j in range(n0 // 2):
        twice_rows(lift[:, tile_of(j)], pairs, j)
    for copy in later:
        copy.wait()
    for r in range(0, tall0, SUB):
        rows = slice(SUB + r, 2 * SUB + r)
        for k in range(n0):
            if r == 0 or r == HALO_Y + ny:
                value = py_in[0 if r == 0 else 1, k]
            else:
                value = p0[1, k, rows, :]
            for i in (0, 1):
                g = side - 1 if i == 0 else side + blocks
                part = pltpu.roll(pk_in[i, r : r + SUB, :], ((g - k) * half0) % LANES, 1)
                value = jnp.where(group == g, part, value)
                if k == (n0 - 1 if i == 0 else 0):
                    g = side - 2 if i == 0 else side + blocks + 1
                    part = pltpu.roll(pk_in[i, r : r + SUB, :], ((g - n0) * half0) % LANES, 1)
                    value = jnp.where(group == g, part, value)
            p0[1, k, rows, :] = value + pairs[k // 2, r : r + SUB, :]
    lv0p.postsmooth(p0, f0q, 0, tiles0, tiles0, False)

    low = SUB + HALO_Y
    body0 = slice(low, low + ny)
    ext = nx + 2 * HALO_X
    for k in range(n0):
        value = lv0p.colours(p0[0, k, body0, :], p0[1, k, body0, :], k)
        slope = [
            p0[1 - c, k, low + 1 : low + 1 + ny, :] - p0[1 - c, k, low - 1 : low - 1 + ny, :] for c in (0, 1)
        ]
        slope = lv0p.colours(slope[0], slope[1], k)
        for e in (0, 1):
            turned, sloped = value[e].T, slope[e].T
            for b in range(side - 1, side + blocks + 1):
                part = slice(b * half0, (b + 1) * half0)
                pn[pl.ds(e * ext + b * n0 + k, half0, stride=2 * ext), :] = turned[part, :]
                if side <= b < side + blocks:
                    gn[pl.ds(e * nx + (b - side) * n0 + k, half0, stride=2 * nx), :] = sloped[part, :]


def finish(nz, nx, predn, pn, gn, wet_in, cor_out, pre_out):
    ext = nx + 2 * HALO_X

    def correct(z):
        for h in range(nx // SUB):
            def cells(dz, dx):
                return pn[pl.ds((z + dz) * ext + HALO_X + h * SUB + dx, SUB), :]

            here = pl.ds(z * nx + h * SUB, SUB)
            pre_out[here, :] = cells(0, 0)
            wet = wet_in[here, :]
            above = cells(1, 0) if z < nz - 1 else 0.0
            below = cells(-1, 0) if z > 0 else 0.0
            slope = (cells(0, 1) - cells(0, -1), gn[here, :], above - below)
            for c in range(3):
                there = pl.ds(c * nz * nx + z * nx + h * SUB, SUB)
                cor_out[there, :] = wet * (predn[there, :] - (0.5 * TIME_STEP) * slope[c])

    for z in range(nz):
        correct(z)


def body(nx_dev, ny_dev, velocity, old_tendency, obstacle):
    _, nz, nx, ny = velocity.shape
    width = nx * nz
    per = LANES // nz
    blocks = nx // per
    tall0 = ny + 2 * HALO_Y
    n1 = nx_dev * (nx // 2) * (nz // 4) // LANES
    tall1 = ny // 2 + 2 * HALO_1
    rows2 = ny_dev * ny // 4
    rows3 = rows2 // 2
    wide2 = 2 * (nx_dev * nx // 4) * (nz // 8)
    tall = max(tall0, tall1, rows2)
    count = max(per // 2, n1 // 2, 1)
    copies = 4 + 14 + 8 + (nx_dev - 1) + 2 * nx_dev + (ny_dev - 1) + 2
    f32 = jnp.float32
    parts = pl.pallas_call(
        functools.partial(kernel, nx_dev, ny_dev, nz, nx, ny),
        out_shape=(
            jax.ShapeDtypeStruct((3 * nz * nx, ny), f32),
            jax.ShapeDtypeStruct((nz * (nx + 2 * HALO_X), ny), f32),
            jax.ShapeDtypeStruct((nz * nx, ny), f32),
            jax.ShapeDtypeStruct((nz * nx, ny), f32),
        ),
        in_specs=[pl.BlockSpec(memory_space=pltpu.HBM)] * 3,
        out_specs=[pl.BlockSpec(memory_space=pltpu.VMEM)] * 4,
        scratch_shapes=[
            pltpu.VMEM((3 * nz * nx, ny), f32),
            pltpu.VMEM((3 * nz * nx, ny), f32),
            pltpu.VMEM((nz * nx, ny), jnp.int32),
            pltpu.VMEM((3, ny + 2 * SUB, width + 2 * LANES), f32),
            pltpu.VMEM((3, ny, width), f32),
            pltpu.VMEM((ny, width), f32),
            pltpu.VMEM((2, 3 * nz, ny), f32),
            pltpu.VMEM((2, 3 * nz, ny), f32),
            pltpu.VMEM((3, ny + 2 * SUB, width + 2 * LANES), f32),
            pltpu.VMEM((2, ny, LANES), f32),
            pltpu.VMEM((2, ny, LANES), f32),
            pltpu.VMEM((2, nz, ny), f32),
            pltpu.VMEM((2, nz, ny), f32),
            pltpu.VMEM((tall0, width + 2 * LANES), f32),
            pltpu.VMEM((blocks + 2, LANES, ny), f32),
            pltpu.VMEM((blocks + 2, LANES, ny), f32),
            pltpu.VMEM((2, per, tall0, LANES), f32),
            pltpu.VMEM((2, per, tall0 + 2 * SUB, LANES), f32),
            pltpu.VMEM((2, ny, LANES), f32),
            pltpu.VMEM((2, tall0, LANES), f32),
            pltpu.VMEM((2, per, SUB, LANES), f32),
            pltpu.VMEM((2, n1, HALO_1, LANES), f32),
            pltpu.VMEM((nx_dev, tall1, LANES), f32),
            pltpu.VMEM((2, n1, tall1, LANES), f32),
            pltpu.VMEM((2, n1, tall1 + 2 * SUB, LANES), f32),
            pltpu.VMEM((rows2, wide2), f32),
            pltpu.VMEM((2, 1, rows2, LANES), f32),
            pltpu.VMEM((2, 1, rows2 + 2 * SUB, LANES), f32),
            pltpu.VMEM((2, 1, rows3, LANES), f32),
            pltpu.VMEM((2, 1, rows3 + 2 * SUB, LANES), f32),
            pltpu.VMEM((count, tall, LANES), f32),
            pltpu.SemaphoreType.DMA((3,)),
            pltpu.SemaphoreType.DMA((copies,)),
            pltpu.SemaphoreType.DMA((copies,)),
        ],
        compiler_params=pltpu.CompilerParams(
            collective_id=0, has_side_effects=True, vmem_limit_bytes=28 * 1024 * 1024
        ),
    )(
        pltpu.with_memory_space_constraint(velocity.reshape(3 * nz * nx, ny), pltpu.HBM),
        pltpu.with_memory_space_constraint(old_tendency.reshape(3 * nz * nx, ny), pltpu.HBM),
        pltpu.with_memory_space_constraint(obstacle.reshape(nz * nx, ny), pltpu.HBM),
    )
    out = pl.pallas_call(
        functools.partial(finish, nz, nx),
        out_shape=(
            jax.ShapeDtypeStruct((3 * nz * nx, ny), f32),
            jax.ShapeDtypeStruct((nz * nx, ny), f32),
        ),
        in_specs=[pl.BlockSpec(memory_space=pltpu.VMEM)] * 4,
        out_specs=[pl.BlockSpec(memory_space=pltpu.VMEM)] * 2,
        compiler_params=pltpu.CompilerParams(vmem_limit_bytes=16 * 1024 * 1024),
    )(*parts)
    return out[0].reshape(3, nz, nx, ny), out[1].reshape(nz, nx, ny)


def solution(mesh):
    placed = (P(None, None, "gx", "gy"), P(None, None, "gx", "gy"), P(None, "gx", "gy"))
    return jax.shard_map(
        functools.partial(body, mesh.shape["gx"], mesh.shape["gy"]),
        mesh=mesh,
        in_specs=placed,
        out_specs=(P(None, None, "gx", "gy"), P(None, "gx", "gy")),
        check_vma=False,
    )
```
